8 devices in a mesh: rep: 1 (over z), data: 2 (over y), expert: 4 (over x, core).
Axes of the slice: x: 2, y: 2, z: 1, core: 2. Of those that a mesh axis runs over, the one named last changes fastest.
Arguments:
- x: bfloat16 [32768, 2048], P(('rep', 'expert', 'data'))
- expert_idx: int32 [32768, 6], P(('rep', 'expert', 'data'))
- gate: float32 [32768, 6], P(('rep', 'expert', 'data'))
- w_gate: bfloat16 [64, 2048, 1408], P('expert', 'data')
- w_up: bfloat16 [64, 2048, 1408], P('expert', 'data')
- w_down: bfloat16 [64, 1408, 2048], P('expert', None, 'data')
Outputs:
- output: bfloat16 [32768, 2048], P(('rep', 'expert', 'data'))
All inputs are finite; a program needn't handle non-finite values.
Results may differ from the reference program's by a relative error of at most 0.00113.
Values are sent between devices in bfloat16 or wider.
A program may use at most 1 GiB of HBM per device.

```python
import jax
import jax.numpy as jnp
from jax import lax

TOK_DEV = 4096
D_MODEL = 2048
FFN = 1408
EXPERTS = 64
TOP_K = 6
EP_SIZE = 4
DP_SIZE = 2
CAPACITY = 480


def route_ids(key):
    n_blocks = EP_SIZE * DP_SIZE
    key_bias, key_hot, key_score = jax.random.split(key, 3)
    expert_bias = jax.random.randint(key_bias, (EXPERTS,), 0, 2 ** 20, dtype=jnp.int32)
    hot_expert = jax.random.randint(key_hot, (), 0, EXPERTS, dtype=jnp.int32)
    scores = jax.random.randint(key_score, (n_blocks, TOK_DEV, EXPERTS), 0, 2 ** 20, dtype=jnp.int32) + expert_bias
    forced = (jnp.arange(TOK_DEV) < CAPACITY)[None, :, None] & (jnp.arange(EXPERTS) == hot_expert)[None, None, :]
    scores = (scores + forced.astype(jnp.int32) * 2 ** 21) * EXPERTS + jnp.arange(EXPERTS, dtype=jnp.int32)
    chosen = lax.top_k(scores, TOP_K)[1]
    return chosen.reshape(n_blocks * TOK_DEV, TOP_K).astype(jnp.int32)


def setup_inputs(seed: int = 0, part: int = 0) -> dict:
    key_shared, key_local = jax.random.split(jax.random.key(seed))
    key_tok, key_route, key_gate = jax.random.split(jax.random.fold_in(key_local, part), 3)
    key_wg, key_wu, key_wd = jax.random.split(key_shared, 3)
    n_rows = EP_SIZE * DP_SIZE * TOK_DEV
    x = jax.random.normal(key_tok, (n_rows, D_MODEL), jnp.float32).astype(jnp.bfloat16)
    gate = jax.random.uniform(key_gate, (n_rows, TOP_K), jnp.float32, 0.2, 0.8)
    w_gate = (jax.random.normal(key_wg, (EXPERTS, D_MODEL, FFN), jnp.float32) * D_MODEL ** -0.5).astype(jnp.bfloat16)
    w_up = (jax.random.normal(key_wu, (EXPERTS, D_MODEL, FFN), jnp.float32) * D_MODEL ** -0.5).astype(jnp.bfloat16)
    w_down = (jax.random.normal(key_wd, (EXPERTS, FFN, D_MODEL), jnp.float32) * (1.5 * FFN ** -0.5)).astype(jnp.bfloat16)
    return {"x": x, "expert_idx": route_ids(key_route), "gate": gate, "w_gate": w_gate, "w_up": w_up, "w_down": w_down}


def slot_table(ids_flat):
    one_hot = (ids_flat[:, None] == jnp.arange(EXPERTS, dtype=jnp.int32)[None, :]).astype(jnp.int32)
    slot_ids = jnp.sum((jnp.cumsum(one_hot, axis=0) - one_hot) * one_hot, axis=1)
    return jnp.where(slot_ids < CAPACITY, ids_flat * CAPACITY + slot_ids, EXPERTS * CAPACITY)


def take_rows(block, index):
    return jnp.take(block, index, axis=0, mode="fill", fill_value=0)


def reference(x, expert_idx, gate, w_gate, w_up, w_down):
    n_blocks = EP_SIZE * DP_SIZE
    x_blocks = x.reshape(n_blocks, TOK_DEV, D_MODEL)
    dest_row = jax.vmap(slot_table)(expert_idx.reshape(n_blocks, TOK_DEV * TOP_K))
    block_ids = jnp.arange(n_blocks)[:, None]
    pair_token = jnp.broadcast_to(jnp.arange(TOK_DEV * TOP_K, dtype=jnp.int32) // TOP_K, dest_row.shape)
    src_tok = jnp.full((n_blocks, EXPERTS * CAPACITY), TOK_DEV, jnp.int32).at[block_ids, dest_row].set(pair_token, mode="drop")
    slot_gate = jnp.zeros((n_blocks, EXPERTS * CAPACITY), jnp.float32).at[block_ids, dest_row].set(gate.reshape(n_blocks, TOK_DEV * TOP_K), mode="drop")
    src_by_exp = src_tok.reshape(n_blocks, EXPERTS, CAPACITY).transpose(1, 0, 2)
    gate_by_exp = slot_gate.reshape(n_blocks, EXPERTS, CAPACITY).transpose(1, 0, 2)

    def expert_step(running, inputs):
        src_e, gate_e, wg_e, wu_e, wd_e = inputs
        expert_rows = jax.vmap(take_rows)(x_blocks, src_e).reshape(n_blocks * CAPACITY, D_MODEL)
        gate_act = jnp.dot(expert_rows, wg_e, preferred_element_type=jnp.float32)
        up_act = jnp.dot(expert_rows, wu_e, preferred_element_type=jnp.float32)
        hidden = (jax.nn.silu(gate_act) * up_act).astype(jnp.bfloat16)
        out_rows = jnp.dot(hidden, wd_e, preferred_element_type=jnp.float32).astype(jnp.bfloat16)
        contrib = out_rows.reshape(n_blocks, CAPACITY, D_MODEL).astype(jnp.float32) * gate_e[:, :, None]
        return running.at[block_ids, src_e].add(contrib, mode="drop"), None

    summed = lax.scan(expert_step, x_blocks.astype(jnp.float32), (src_by_exp, gate_by_exp, w_gate, w_up, w_down))[0]
    return summed.astype(jnp.bfloat16).reshape(n_blocks * TOK_DEV, D_MODEL)
```

```python
import functools

import jax
import jax.numpy as jnp
from jax import lax
from jax.experimental import pallas as pl
from jax.experimental.pallas import tpu as pltpu
from jax.sharding import PartitionSpec as P


LANES = 128
NO_EXPERT = LANES - 1
TILE = 256
WINDOW = 128
MOVES = 2
TAIL, TAIL_CAP = 3, 16
BF16, F32, I32 = jnp.bfloat16, jnp.float32, jnp.int32
ANY = pl.BlockSpec(memory_space=pl.ANY)
SMEM = pl.BlockSpec(memory_space=pltpu.SMEM)
VMEM_LIMIT = 62 * 1024 * 1024
TOKEN = jax.ShapeDtypeStruct((1,), I32)


def capacity_rows(tok_rows, top_k, n_exp):
    return max(8, ((5 * top_k * tok_rows) // (4 * n_exp) + 7) // 8 * 8)


def params(n_axes=0):
    return pltpu.CompilerParams(dimension_semantics=("arbitrary",) * n_axes if n_axes else None, vmem_limit_bytes=VMEM_LIMIT)


def cost(flops, bytes_accessed):
    return pl.CostEstimate(flops=flops, bytes_accessed=bytes_accessed, transcendentals=0)


def route_body(capacity, ids_ref, gate_ref, slot_ref, slot_t_ref, gate_te_ref, start_ref, count_ref, seen):
    @pl.when(pl.program_id(0) == 0)
    def _():
        seen[...] = jnp.zeros_like(seen)

    top_k, tile = ids_ref.shape
    expert = lax.broadcasted_iota(I32, (LANES, tile), 0)
    mask = jnp.zeros((LANES, tile), F32)
    gate_t = jnp.zeros((LANES, tile), F32)
    for j in range(top_k):
        hit = ids_ref[j : j + 1, :] == expert
        mask = jnp.where(hit, 1.0, mask)
        gate_t = jnp.where(hit, gate_ref[j : j + 1, :], gate_t)
    before = lax.broadcasted_iota(I32, (tile, tile), 0) < lax.broadcasted_iota(I32, (tile, tile), 1)
    earlier = jnp.dot(mask.astype(BF16), jnp.where(before, 1.0, 0.0).astype(BF16), preferred_element_type=F32) + seen[:, 0:1]
    slot = jnp.where((mask > 0.0) & (earlier < capacity), earlier, -1.0)
    slot_t_ref[...] = slot.astype(I32)
    slot_ref[...] = slot.T.astype(I32)
    gate_te_ref[...] = gate_t.T
    start_ref[0] = jnp.minimum(seen[...].T[:8], capacity).astype(I32)
    seen[...] = seen[...] + jnp.sum(mask, axis=1, keepdims=True)
    count_ref[...] = jnp.minimum(seen[...].T[:8], capacity).astype(I32)


def route(ids_t, gate_t, capacity):
    top_k, tok_rows = ids_t.shape
    n_tiles = tok_rows // TILE
    col = pl.BlockSpec((TILE, LANES), lambda i: (i, 0))
    return pl.pallas_call(
        functools.partial(route_body, capacity),
        grid=(n_tiles,),
        in_specs=[pl.BlockSpec((top_k, TILE), lambda i: (0, i))] * 2,
        out_specs=[
            col,
            pl.BlockSpec((LANES, TILE), lambda i: (0, i)),
            col,
            pl.BlockSpec((1, 8, LANES), lambda i: (i, 0, 0)),
            pl.BlockSpec((8, LANES), lambda i: (0, 0)),
        ],
        out_shape=[
            jax.ShapeDtypeStruct((tok_rows, LANES), I32),
            jax.ShapeDtypeStruct((LANES, tok_rows), I32),
            jax.ShapeDtypeStruct((tok_rows, LANES), F32),
            jax.ShapeDtypeStruct((n_tiles, 8, LANES), I32),
            jax.ShapeDtypeStruct((8, LANES), I32),
        ],
        scratch_shapes=[pltpu.VMEM((LANES, LANES), F32)],
        compiler_params=params(1),
        name="route",
    )(ids_t, gate_t)


def windows(start_ref, tile, e, capacity, step):
    lo, hi = start_ref[tile, e], start_ref[tile + 1, e]
    floor = lo // 16 * 16
    n_win = jnp.where(hi > lo, (hi - floor + WINDOW - 1) // WINDOW, 0)

    @pl.loop(0, n_win)
    def _(w):
        first = floor + w * WINDOW
        step(first, pl.multiple_of(jnp.minimum(first, capacity - WINDOW), 16))


def pick_body(r_ref, tab_ref, start_ref, slot_t_ref, x_ref, *refs):
    outs, token = refs[:-1], refs[-1]
    tile = pl.program_id(0)
    token[0] = 0

    @pl.when(tile == 0)
    def _():
        for out in outs:
            out[...] = jnp.zeros_like(out)

    for k, out in enumerate(outs):
        e = tab_ref[r_ref[0] + 1, k]

        def step(first, base, out=out, e=e):
            slots = slot_t_ref[pl.ds(e, 1), :]
            row = lax.broadcasted_iota(I32, (WINDOW, TILE), 0) + base
            hot = jnp.where((row == slots) & (slots >= first), 1.0, 0.0).astype(BF16)
            out[pl.ds(base, WINDOW), :] += jnp.dot(hot, x_ref[...], preferred_element_type=F32).astype(BF16)

        windows(start_ref, tile, e, out.shape[0], step)


def pick(r, table, starts, slot_t, x_loc, capacity):
    n_pick = table.shape[1]
    tok_rows, d_model = x_loc.shape
    return pl.pallas_call(
        pick_body,
        grid=(tok_rows // TILE,),
        in_specs=[
            SMEM,
            SMEM,
            SMEM,
            pl.BlockSpec((LANES, TILE), lambda i: (0, i)),
            pl.BlockSpec((TILE, d_model), lambda i: (i, 0)),
        ],
        out_specs=[pl.BlockSpec((capacity, d_model), lambda i: (0, 0))] * n_pick + [SMEM],
        out_shape=[jax.ShapeDtypeStruct((capacity, d_model), BF16)] * n_pick + [TOKEN],
        compiler_params=params(1),
        cost_estimate=cost(2 * n_pick * capacity * TILE * d_model, 2 * tok_rows * d_model),
        name="pick",
    )(r, table, starts, slot_t, x_loc)


def pick_tail_body(tail_ref, slot_t_ref, x_ref, *outs):
    tile = pl.program_id(0)
    n_tail = tail_ref.shape[1]
    group = n_tail * TAIL_CAP
    hots = []
    for k in range(len(outs)):
        for i in range(n_tail):
            row = lax.broadcasted_iota(I32, (TAIL_CAP, x_ref.shape[0]), 0)
            hots.append(jnp.where(row == slot_t_ref[pl.ds(tail_ref[k, i], 1), :], 1.0, 0.0).astype(BF16))
    picked = jnp.dot(jnp.concatenate(hots, axis=0), x_ref[...], preferred_element_type=F32).astype(BF16)

    @pl.when(tile == 0)
    def _():
        for out in outs:
            out[...] = jnp.zeros_like(out)

    for k, out in enumerate(outs):
        out[...] += picked[k * group : (k + 1) * group]


def pick_tail(tail, slot_t, x_loc):
    n_pos, n_tail = tail.shape
    tok_rows, d_model = x_loc.shape
    group = n_tail * TAIL_CAP
    return pl.pallas_call(
        pick_tail_body,
        grid=(tok_rows // TILE,),
        in_specs=[SMEM, pl.BlockSpec((LANES, TILE), lambda i: (0, i)), pl.BlockSpec((TILE, d_model), lambda i: (i, 0))],
        out_specs=[pl.BlockSpec((group, d_model), lambda i: (0, 0))] * n_pos,
        out_shape=[jax.ShapeDtypeStruct((group, d_model), BF16)] * n_pos,
        compiler_params=params(1),
        cost_estimate=cost(2 * n_pos * group * tok_rows * d_model, 2 * tok_rows * d_model),
        name="pick_tail",
    )(tail, slot_t, x_loc)


def ffn_body(n_local, r_ref, src_ref, used_ref, *refs):
    n_src = 1 + MOVES
    own, (pg, pu, pd) = refs[: 3 * n_src], refs[3 * n_src : 3 * n_src + 3]
    refs = refs[3 * n_src + 3 :]
    n_rows = used_ref.shape[1]
    rows, outs, token = refs[:n_rows], refs[n_rows : 2 * n_rows], refs[2 * n_rows]
    x_buf, w_in, w_out, o_buf, x_sem, w_sem, o_sem = refs[2 * n_rows + 1 :]
    half, ffn = pg.shape
    q = lax.axis_index("data")
    r = r_ref[0]
    src = src_ref[r]
    token[0] = 0

    def load(place, parts, first):
        at = pl.ds(pl.multiple_of(place * half, half), half)
        places = (w_in.at[at, pl.ds(0, ffn)], w_in.at[at, pl.ds(ffn, ffn)], w_out.at[:, at])
        return [pltpu.make_async_copy(part, dst, w_sem.at[first + i]) for i, (part, dst) in enumerate(zip(parts, places))]

    row_loads = [pltpu.make_async_copy(rows[i], x_buf.at[i], x_sem.at[i]) for i in range(n_rows)]
    row_loads[0].start()
    theirs = load(1 - q, (pg, pu, pd), 3)
    for copy in theirs[:2]:
        copy.start()
    for s in range(n_src):
        @pl.when(jnp.maximum(src - n_local + 1, 0) == s)
        def _():
            parts = own[3 * s : 3 * s + 3]
            for copy in load(q, [part.at[jnp.minimum(src, n_local - 1)] for part in parts] if s == 0 else parts, 0):
                copy.start()
    theirs[2].start()
    for copy in row_loads[1:]:
        copy.start()
    ours = load(q, (pg, pu, pd), 0)
    for copy in row_loads + ours + theirs:
        copy.wait()

    n_part = 2
    part = x_buf.shape[1] // n_part

    @pl.loop(0, n_rows)
    def _(i):
        @pl.loop(0, n_part)
        def _(j):
            at = pl.ds(pl.multiple_of(j * part, part), part)

            @pl.when(used_ref[r, i] > j * part)
            def _():
                act = jnp.dot(x_buf[i, at], w_in[...], preferred_element_type=F32)
                gate_act, up_act = act[:, :ffn], act[:, ffn:]
                hidden = (jax.nn.silu(gate_act) * up_act).astype(BF16)
                o_buf[i, at] = jnp.dot(hidden, w_out[...], preferred_element_type=F32).astype(BF16)

            @pl.when(used_ref[r, i] <= j * part)
            def _():
                o_buf[i, at] = jnp.zeros((part, o_buf.shape[2]), BF16)

        for s in range(n_rows):
            @pl.when(i == s)
            def _():
                pltpu.make_async_copy(o_buf.at[s], outs[s], o_sem.at[s]).start()

    for s in range(n_rows):
        pltpu.make_async_copy(o_buf.at[s], outs[s], o_sem.at[s]).wait()


def expert_ffn(r, sources, used, weights, extras, peer, rows):
    capacity, d_model = rows[0].shape
    n_local, half, ffn = weights[0].shape
    n_rows = len(rows)
    own = list(weights) + [part for extra in extras for part in extra]
    out = pl.pallas_call(
        functools.partial(ffn_body, n_local),
        in_specs=[SMEM] * 3 + [ANY] * (len(own) + 3 + n_rows),
        out_specs=[ANY] * n_rows + [SMEM],
        out_shape=[jax.ShapeDtypeStruct((capacity, d_model), BF16)] * n_rows + [TOKEN],
        scratch_shapes=[
            pltpu.VMEM((n_rows, capacity, d_model), BF16),
            pltpu.VMEM((2 * half, 2 * ffn), BF16),
            pltpu.VMEM((ffn, d_model), BF16),
            pltpu.VMEM((n_rows, capacity, d_model), BF16),
            pltpu.SemaphoreType.DMA((n_rows,)),
            pltpu.SemaphoreType.DMA((6,)),
            pltpu.SemaphoreType.DMA((n_rows,)),
        ],
        compiler_params=params(),
        cost_estimate=cost(6 * n_rows * capacity * d_model * ffn, 6 * d_model * ffn),
        name="ffn",
    )(r, sources, used, *own, *peer, *rows)
    return tuple(out[:n_rows]), out[n_rows]


def tail_sum(tail_ref, slot_ref, gate_ref, rows_ref, total):
    n_pos, n_tail = tail_ref.shape
    n_col = rows_ref.shape[0]
    row = lax.broadcasted_iota(I32, (LANES, n_col), 0)
    group = lax.broadcasted_iota(I32, (LANES, n_col), 1) // TAIL_CAP
    wanted = jnp.full((LANES, n_col), NO_EXPERT, I32)
    for k in range(n_pos):
        for i in range(n_tail):
            wanted = jnp.where(group == k * n_tail + i, tail_ref[k, i], wanted)
    select = jnp.where(row == wanted, 1.0, 0.0).astype(BF16)
    slots = jnp.dot(slot_ref[...].astype(F32).astype(BF16), select, preferred_element_type=F32)
    place = lax.broadcasted_iota(I32, (TILE, n_col), 1) % TAIL_CAP
    here = slots == place.astype(F32)
    rest = gate_ref[...]
    weights = []
    for _ in range(3):
        piece = rest.astype(BF16)
        rest = rest - piece.astype(F32)
        weights.append(jnp.where(here, jnp.dot(piece, select, preferred_element_type=F32), 0.0).astype(BF16))
    parts = jnp.dot(jnp.concatenate(weights, axis=0), rows_ref[...], preferred_element_type=F32)
    total[...] += parts[:TILE] + parts[TILE : 2 * TILE] + parts[2 * TILE :]


def mix_body(has_tail, r_ref, tab_ref, start_ref, slot_ref, gate_ref, *refs):
    n_rows = tab_ref.shape[1]
    rows, refs = refs[:n_rows], refs[n_rows:]
    acc_ref, tails, (out_ref, token, total) = refs[0], refs[1:-3], refs[-3:]
    tile = pl.program_id(0)
    token[0] = 0
    total[...] = acc_ref[...]
    if has_tail:
        tail_sum(tails[0], slot_ref, gate_ref, tails[1], total)
    lane = lax.broadcasted_iota(I32, (TILE, LANES), 1)
    for k in range(n_rows):
        e = tab_ref[r_ref[0] + 1, k]

        def step(first, base, k=k, e=e):
            here = lane == e
            slots = jnp.max(jnp.where(here, slot_ref[...], -1), axis=1, keepdims=True)
            gates = jnp.sum(jnp.where(here, gate_ref[...], 0.0), axis=1, keepdims=True)
            column = lax.broadcasted_iota(I32, (TILE, WINDOW), 1) + base
            hot = jnp.where((column == slots) & (slots >= first), 1.0, 0.0).astype(BF16)
            total[...] += gates * jnp.dot(hot, rows[k][pl.ds(base, WINDOW), :], preferred_element_type=F32)

        windows(start_ref, tile, e, rows[k].shape[0], step)
    out_ref[...] = total[...].astype(out_ref.dtype)


def mix(r, table, starts, slot, gate_te, rows, acc, out_dtype, tail=()):
    _, d_model = rows[0].shape
    tok_rows = acc.shape[0]
    n_rows = len(rows)
    col = pl.BlockSpec((TILE, LANES), lambda i: (i, 0))
    wide = pl.BlockSpec((TILE, d_model), lambda i: (i, 0))

    def held(value):
        return pl.BlockSpec(value.shape, lambda i: (0, 0), pipeline_mode=pl.Buffered(1))

    return pl.pallas_call(
        functools.partial(mix_body, bool(tail)),
        grid=(tok_rows // TILE,),
        in_specs=[SMEM, SMEM, SMEM, col, col] + [held(row) for row in rows] + [wide] + ([SMEM, held(tail[1])] if tail else []),
        out_specs=[wide, SMEM],
        out_shape=[jax.ShapeDtypeStruct((tok_rows, d_model), out_dtype), TOKEN],
        scratch_shapes=[pltpu.VMEM((TILE, d_model), F32)],
        input_output_aliases={5 + n_rows: 0} if acc.dtype == out_dtype else {},
        compiler_params=params(1),
        cost_estimate=cost(2 * n_rows * tok_rows * WINDOW * d_model, 8 * tok_rows * d_model),
        name="mix",
    )(r, table, starts, slot, gate_te, *rows, acc, *tail)


def tail_in_body(idx_ref, x_ref, wg_ref, wu_ref, out_ref):
    n_src, _, rows, half = x_ref.shape
    ffn = wg_ref.shape[2]
    x = x_ref[...].reshape(n_src * rows, half)
    out_ref[:, 0, :, :ffn] = jnp.dot(x, wg_ref[0], preferred_element_type=F32).reshape(n_src, rows, ffn)
    out_ref[:, 0, :, ffn:] = jnp.dot(x, wu_ref[0], preferred_element_type=F32).reshape(n_src, rows, ffn)


def tail_in(idx, x, w_gate, w_up):
    n_src, n_tail, rows, half = x.shape
    ffn = w_gate.shape[2]
    weight = pl.BlockSpec((1, half, ffn), lambda i, idx: (idx[i], 0, 0))
    return pl.pallas_call(
        tail_in_body,
        grid_spec=pltpu.PrefetchScalarGridSpec(
            num_scalar_prefetch=1,
            grid=(n_tail,),
            in_specs=[pl.BlockSpec((n_src, 1, rows, half), lambda i, idx: (0, i, 0, 0)), weight, weight],
            out_specs=pl.BlockSpec((n_src, 1, rows, 2 * ffn), lambda i, idx: (0, i, 0, 0)),
        ),
        out_shape=jax.ShapeDtypeStruct((n_src, n_tail, rows, 2 * ffn), F32),
        compiler_params=params(1),
        cost_estimate=cost(4 * n_src * n_tail * rows * half * ffn, 4 * n_tail * half * ffn),
        name="tail_in",
    )(idx, x, w_gate, w_up)


def tail_out_body(idx_ref, h_ref, wd_ref, out_ref):
    n_src, _, rows, ffn = h_ref.shape
    out = jnp.dot(h_ref[...].reshape(n_src * rows, ffn), wd_ref[0], preferred_element_type=F32)
    out_ref[:, 0] = out.reshape(n_src, rows, -1).astype(BF16)


def tail_out(idx, hidden, w_down):
    n_src, n_tail, rows, ffn = hidden.shape
    half = w_down.shape[2]
    return pl.pallas_call(
        tail_out_body,
        grid_spec=pltpu.PrefetchScalarGridSpec(
            num_scalar_prefetch=1,
            grid=(n_tail,),
            in_specs=[
                pl.BlockSpec((n_src, 1, rows, ffn), lambda i, idx: (0, i, 0, 0)),
                pl.BlockSpec((1, ffn, half), lambda i, idx: (idx[i], 0, 0)),
            ],
            out_specs=pl.BlockSpec((n_src, 1, rows, half), lambda i, idx: (0, i, 0, 0)),
        ),
        out_shape=jax.ShapeDtypeStruct((n_src, n_tail, rows, half), BF16),
        compiler_params=params(1),
        cost_estimate=cost(2 * n_src * n_tail * rows * half * ffn, 2 * n_tail * half * ffn),
        name="tail_out",
    )(idx, hidden, w_down)


def plan(counts, n_group):
    load = jnp.max(counts, axis=0).reshape(n_group, -1)
    n_local = load.shape[1]
    ids = jnp.arange(n_local, dtype=I32)
    ahead = (load[:, None, :] > load[:, :, None]) | ((load[:, None, :] == load[:, :, None]) & (ids[None, None, :] < ids[None, :, None]))
    rank = jnp.sum(ahead.astype(I32), axis=2)
    active = jnp.sum((load > 0).astype(I32), axis=1)
    tail = jnp.minimum(jnp.sum(((load > 0) & (load <= TAIL_CAP)).astype(I32), axis=1), TAIL)
    full = active - tail
    partner = full.reshape(-1, 2)[:, ::-1].reshape(-1)
    give = jnp.clip((full - partner) // 2, 0, MOVES)
    keep = full - give
    partner_keep = keep.reshape(-1, 2)[:, ::-1].reshape(-1)
    position = jnp.arange(n_group, dtype=I32)[:, None]
    kept = rank < keep[:, None]
    in_round = rank < full[:, None]
    to = jnp.where(kept, position, position ^ 1)
    at = jnp.where(kept, rank, partner_keep[:, None] + rank - keep[:, None])
    source = jnp.where(kept, ids[None, :], n_local + rank - keep[:, None])
    tail_at = jnp.where((rank >= full[:, None]) & (rank < active[:, None]), rank - full[:, None], -1)
    n_slots = n_local + MOVES + 2
    flat = lambda a: jnp.broadcast_to(a, load.shape).reshape(-1)
    expert = jnp.arange(load.size, dtype=I32)
    rounds = jnp.arange(n_slots, dtype=I32)
    hit = (flat(to)[None, None, :] == position[:, :, None]) & (flat(at)[None, None, :] == rounds[None, :, None]) & flat(in_round)[None, None, :]
    table = jnp.max(jnp.where(hit, (expert + LANES * flat(source))[None, None, :], -1), axis=2)
    experts = jnp.where(table < 0, NO_EXPERT, table % LANES)
    sources = jnp.where(table < 0, 0, table // LANES)
    steps = jnp.arange(max(TAIL, MOVES), dtype=I32)
    tail_hit = tail_at[:, None, :] == steps[None, :TAIL, None]
    tails = jnp.max(jnp.where(tail_hit, ids[None, None, :], -1), axis=2)
    move_hit = (rank - keep[:, None])[:, None, :] == steps[None, :MOVES, None]
    moves = jnp.max(jnp.where(move_hit, ids[None, None, :], 0), axis=2)
    return experts, sources, tails, moves, jnp.maximum(jnp.max(keep + give.reshape(-1, 2)[:, ::-1].reshape(-1)), 1)


def solution(mesh):
    n_group, n_data = mesh.shape["expert"], mesh.shape["data"]
    assert n_group == 4 and n_data == 2
    tok_spec = P(("rep", "expert", "data"), None)
    wide_spec = P("expert", "data", None)
    down_spec = P("expert", None, "data")
    swap = [(0, 1), (1, 0)]

    def across(value, k):
        return lax.ppermute(value, "expert", [(p, p ^ k) for p in range(n_group)])

    def spread(groups):
        return (groups[0],) + tuple(across(groups[k], k) for k in range(1, n_group))

    def swapped(parts):
        return tuple(lax.ppermute(part, "data", swap) for part in parts)

    def device_body(x_loc, idx_loc, gate_loc, wg_loc, wu_loc, wd_loc):
        tok_rows, d_model = x_loc.shape
        top_k = idx_loc.shape[1]
        n_local = wg_loc.shape[0]
        n_exp = n_local * n_group
        capacity = capacity_rows(tok_rows, top_k, n_exp)
        me, q = lax.axis_index("expert"), lax.axis_index("data")
        weights = (wg_loc, wu_loc, wd_loc)
        slot, slot_t, gate_te, tile_starts, count = route(idx_loc.T, gate_loc.T, capacity)
        starts = jnp.concatenate([tile_starts[:, 0], count[:1]], axis=0)
        counts = lax.all_gather(count[0, :n_exp], ("expert", "data"))
        experts, sources, tails, moves, n_round = plan(counts, n_group)
        mine = me ^ jnp.arange(n_group, dtype=I32)
        table = jnp.concatenate([jnp.full((1, n_group), NO_EXPERT, I32), experts[mine].T], axis=0)
        my_sources = sources[me]
        my_hot = (experts[me][:, None] == jnp.arange(n_exp, dtype=I32)[None, :]).astype(I32)
        my_counts = counts.reshape(n_group, n_data, n_exp)[mine, q]
        used = jnp.sum(my_hot[:, None, :] * my_counts[None, :, :], axis=2)
        tail_local = jnp.maximum(tails[me], 0)
        tail_global = jnp.where(tails < 0, NO_EXPERT, tails + n_local * jnp.arange(n_group, dtype=I32)[:, None])[mine]

        def slices(e, source=None):
            return tuple(lax.dynamic_index_in_dim(w, e, axis=0, keepdims=False) for w in source or weights)

        def outgoing(r):
            s = my_sources[r]
            kind = jnp.maximum(s - n_local + 1, 0)
            return lax.switch(kind, [lambda: slices(jnp.minimum(s, n_local - 1))] + [lambda i=i: extras[i] for i in range(MOVES)])

        def one_round(r, carry):
            token, peer, rows, back, send, acc = carry
            peer_next = swapped(send)
            *picked, token = pick(r + 1 + token, table, starts, slot_t, x_loc, capacity)
            rows_next = spread(picked)
            out_rows, token = expert_ffn(r + token, my_sources, used, weights, extras, peer, rows)
            back_next = spread(out_rows)
            send_next, token = lax.optimization_barrier((outgoing(r[0] + 2 + token[0]), token))
            acc, token = mix(r - 1 + token, table, starts, slot, gate_te, back, acc, F32)
            return token, peer_next, rows_next, back_next, send_next, acc

        peer = swapped(slices(my_sources[0]))
        *picked, token = pick(jnp.zeros((1,), I32), table, starts, slot_t, x_loc, capacity)
        rows = spread(picked)
        later, token = lax.optimization_barrier((weights, token))
        extras = tuple(tuple(across(part, 1) for part in slices(moves[me, i] + token[0], later)) for i in range(MOVES))
        send, token = lax.optimization_barrier((outgoing(1 + token[0]), token))
        tail_rows = spread(pick_tail(tail_global + token, slot_t, x_loc))
        blank = tuple(jnp.zeros((capacity, d_model), BF16) for _ in range(n_group))
        carry = (token, peer, rows, blank, send, x_loc.astype(F32))
        tail_x = jnp.stack([rows.reshape(TAIL, TAIL_CAP, d_model) for rows in tail_rows], axis=1).reshape(TAIL, n_group * TAIL_CAP, d_model)
        half = d_model // n_data
        tail_mine = lax.dynamic_slice_in_dim(tail_x, q * half, half, axis=2)
        tail_peer = lax.ppermute(lax.dynamic_slice_in_dim(tail_x, (1 - q) * half, half, axis=2), "data", swap)

        odd = (n_round - 1) % 2
        carry = lax.fori_loop(0, odd, lambda i, c: one_round(jnp.full((1,), i, I32), c), carry)

        def two_rounds(i, c):
            r = jnp.full((1,), odd + 2 * i, I32)
            return one_round(r + 1, one_round(r, c))

        token, peer, rows, back, _, acc = lax.fori_loop(0, (n_round - 1) // 2, two_rounds, carry)
        last = jnp.full((1,), n_round - 1, I32)
        partial = tail_in(tail_local + token, jnp.stack([tail_mine, tail_peer]), wg_loc, wu_loc)
        partial, token = lax.optimization_barrier((partial, token))
        partial_sum = partial[0] + lax.ppermute(partial[1], "data", swap)
        out_last, token = expert_ffn(last + token, my_sources, used, weights, extras, peer, rows)
        back_last = spread(out_last)
        acc, token = mix(last - 1 + token, table, starts, slot, gate_te, back, acc, F32)
        ffn = wg_loc.shape[2]
        tail_h = (jax.nn.silu(partial_sum[..., :ffn]) * partial_sum[..., ffn:]).astype(BF16)
        tail_o = tail_out(tail_local + token, jnp.stack([tail_h, lax.ppermute(tail_h, "data", swap)]), wd_loc)
        other_half = lax.ppermute(tail_o[1], "data", swap)
        whole = jnp.where(q == 0, jnp.concatenate([tail_o[0], other_half], axis=2), jnp.concatenate([other_half, tail_o[0]], axis=2))
        whole = whole.reshape(TAIL, n_group, TAIL_CAP, d_model)
        tail_back = spread([whole[:, k].reshape(TAIL * TAIL_CAP, d_model) for k in range(n_group)])
        tail = (tail_global, jnp.concatenate(tail_back, axis=0))
        return mix(last + token, table, starts, slot, gate_te, back_last, acc, BF16, tail)[0]

    return jax.shard_map(device_body, mesh=mesh, in_specs=(tok_spec, tok_spec, tok_spec, wide_spec, wide_spec, down_spec), out_specs=tok_spec, check_vma=False)
```

```python
import functools

import jax
import jax.numpy as jnp
from jax import lax
from jax.experimental import pallas as pl
from jax.experimental.pallas import tpu as pltpu
from jax.sharding import PartitionSpec as P


LANES = 128
NO_EXPERT = LANES - 1
TILE = 256
WINDOW = 128
MIX_WINDOW = 64
MIX_STRIP = 512
AHEAD = 4
MOVES = 2
LIGHT = 160
TAIL, TAIL_CAP = 3, 16
BF16, F32, I32 = jnp.bfloat16, jnp.float32, jnp.int32
ANY = pl.BlockSpec(memory_space=pl.ANY)
SMEM = pl.BlockSpec(memory_space=pltpu.SMEM)
VMEM_LIMIT = 62 * 1024 * 1024
TOKEN = jax.ShapeDtypeStruct((1,), I32)


def capacity_rows(tok_rows, top_k, n_exp):
    return max(8, ((5 * top_k * tok_rows) // (4 * n_exp) + 7) // 8 * 8)


def params(n_axes=0):
    return pltpu.CompilerParams(dimension_semantics=("arbitrary",) * n_axes if n_axes else None, vmem_limit_bytes=VMEM_LIMIT)


def cost(flops, bytes_accessed):
    return pl.CostEstimate(flops=flops, bytes_accessed=bytes_accessed, transcendentals=0)


def route_body(capacity, ids_ref, gate_ref, pieces_ref, slot_t_ref, start_ref, count_ref, seen):
    @pl.when(pl.program_id(0) == 0)
    def _():
        seen[...] = jnp.zeros_like(seen)

    top_k, tile = ids_ref.shape[0], TILE
    tokens = pl.ds(pl.multiple_of(pl.program_id(0) * TILE, TILE), TILE)
    ids, gates = ids_ref[:, tokens], gate_ref[:, tokens]
    expert = lax.broadcasted_iota(I32, (LANES, tile), 0)
    mask = jnp.zeros((LANES, tile), F32)
    gate_t = jnp.zeros((LANES, tile), F32)
    for j in range(top_k):
        hit = ids[j : j + 1, :] == expert
        mask = jnp.where(hit, 1.0, mask)
        gate_t = jnp.where(hit, gates[j : j + 1, :], gate_t)
    before = lax.broadcasted_iota(I32, (tile, tile), 0) < lax.broadcasted_iota(I32, (tile, tile), 1)
    earlier = jnp.dot(mask.astype(BF16), jnp.where(before, 1.0, 0.0).astype(BF16), preferred_element_type=F32) + seen[:, 0:1]
    slot = jnp.where((mask > 0.0) & (earlier < capacity), earlier, -1.0)
    slot_t_ref[...] = slot.astype(I32)
    slot = slot.T
    high = jnp.floor(slot * (1.0 / 16.0))
    pieces = [high.astype(BF16), (slot - 16.0 * high).astype(BF16)]
    rest = gate_t.T
    for _ in range(3):
        piece = rest.astype(BF16)
        rest = rest - piece.astype(F32)
        pieces.append(piece)
    for i, piece in enumerate(pieces):
        pieces_ref[:, i * LANES : (i + 1) * LANES] = piece
    start_ref[0] = jnp.minimum(seen[...].T[:8], capacity).astype(I32)
    seen[...] = seen[...] + jnp.sum(mask, axis=1, keepdims=True)
    count_ref[...] = jnp.minimum(seen[...].T[:8], capacity).astype(I32)


def route(ids_t, gate_t, capacity):
    top_k, tok_rows = ids_t.shape
    n_tiles = tok_rows // TILE
    return pl.pallas_call(
        functools.partial(route_body, capacity),
        grid=(n_tiles,),
        in_specs=[pl.BlockSpec((top_k, tok_rows), lambda i: (0, 0))] * 2,
        out_specs=[
            pl.BlockSpec((TILE, 5 * LANES), lambda i: (i, 0)),
            pl.BlockSpec((LANES, TILE), lambda i: (0, i)),
            pl.BlockSpec((1, 8, LANES), lambda i: (i, 0, 0)),
            pl.BlockSpec((8, LANES), lambda i: (0, 0)),
        ],
        out_shape=[
            jax.ShapeDtypeStruct((tok_rows, 5 * LANES), BF16),
            jax.ShapeDtypeStruct((LANES, tok_rows), I32),
            jax.ShapeDtypeStruct((n_tiles, 8, LANES), I32),
            jax.ShapeDtypeStruct((8, LANES), I32),
        ],
        scratch_shapes=[pltpu.VMEM((LANES, LANES), F32)],
        compiler_params=params(1),
        name="route",
    )(ids_t, gate_t)


def windows(start_ref, tile, e, width):
    lo, hi = start_ref[tile, e], start_ref[tile + 1, e]
    floor = lo // 16 * 16
    return floor, jnp.where(hi > lo, (hi - floor + width - 1) // width, 0)


def stream_rows(tile, x_hbm, x_buf, sem):
    def copy(i):
        at = pl.ds(pl.multiple_of(i * TILE, TILE), TILE)
        return pltpu.make_async_copy(x_hbm.at[at], x_buf.at[at], sem.at[i])

    @pl.when(tile == 0)
    def _():
        @pl.loop(0, pl.num_programs(0))
        def _(i):
            copy(i).start()

    copy(tile).wait()
    return x_buf.at[pl.ds(pl.multiple_of(tile * TILE, TILE), TILE)]


def pick_body(r_ref, tab_ref, start_ref, slot_t_ref, x_hbm, *refs):
    *outs, token, picked, sem, x_buf, x_sem = refs
    n_pick, capacity, _ = picked.shape
    tile = pl.program_id(0)
    token[0] = 0

    x_ref = stream_rows(tile, x_hbm, x_buf, x_sem)

    @pl.when(tile == 0)
    def _():
        picked[...] = jnp.zeros_like(picked)

    @pl.loop(0, n_pick)
    def _(k):
        e = tab_ref[r_ref[0] + 1, k]
        floor, n_win = windows(start_ref, tile, e, WINDOW)

        @pl.loop(0, n_win)
        def _(w):
            first = floor + w * WINDOW
            base = pl.multiple_of(jnp.minimum(first, capacity - WINDOW), 16)
            slots = slot_t_ref[pl.ds(e, 1), :]
            row = lax.broadcasted_iota(I32, (WINDOW, TILE), 0) + base
            hot = jnp.where((row == slots) & (slots >= first), 1.0, 0.0).astype(BF16)
            picked[k, pl.ds(base, WINDOW), :] += jnp.dot(hot, x_ref[...], preferred_element_type=F32).astype(BF16)

    @pl.when(tile == pl.num_programs(0) - 1)
    def _():
        copies = [pltpu.make_async_copy(picked.at[k], out, sem.at[k]) for k, out in enumerate(outs)]
        for copy in copies:
            copy.start()
        for copy in copies:
            copy.wait()


def pick(r, table, starts, slot_t, x_loc, capacity):
    n_pick = table.shape[1]
    tok_rows, d_model = x_loc.shape
    return pl.pallas_call(
        pick_body,
        grid=(tok_rows // TILE,),
        in_specs=[
            SMEM,
            SMEM,
            SMEM,
            pl.BlockSpec((LANES, TILE), lambda i: (0, i)),
            ANY,
        ],
        out_specs=[ANY] * n_pick + [SMEM],
        out_shape=[jax.ShapeDtypeStruct((capacity, d_model), BF16)] * n_pick + [TOKEN],
        scratch_shapes=[
            pltpu.VMEM((n_pick, capacity, d_model), BF16),
            pltpu.SemaphoreType.DMA((n_pick,)),
            pltpu.VMEM((tok_rows, d_model), BF16),
            pltpu.SemaphoreType.DMA((tok_rows // TILE,)),
        ],
        compiler_params=params(1),
        cost_estimate=cost(2 * n_pick * capacity * TILE * d_model, 2 * tok_rows * d_model),
        name="pick",
    )(r, table, starts, slot_t, x_loc)


def pick_tail_body(tail_ref, slot_t_ref, x_hbm, *refs):
    *outs, x_buf, x_sem = refs
    tile = pl.program_id(0)
    x_ref = stream_rows(tile, x_hbm, x_buf, x_sem)
    n_tail = tail_ref.shape[1]
    group = n_tail * TAIL_CAP
    hots = []
    for k in range(len(outs)):
        for i in range(n_tail):
            row = lax.broadcasted_iota(I32, (TAIL_CAP, x_ref.shape[0]), 0)
            hots.append(jnp.where(row == slot_t_ref[pl.ds(tail_ref[k, i], 1), :], 1.0, 0.0).astype(BF16))
    picked = jnp.dot(jnp.concatenate(hots, axis=0), x_ref[...], preferred_element_type=F32).astype(BF16)

    @pl.when(tile == 0)
    def _():
        for out in outs:
            out[...] = jnp.zeros_like(out)

    for k, out in enumerate(outs):
        out[...] += picked[k * group : (k + 1) * group]


def pick_tail(tail, slot_t, x_loc):
    n_pos, n_tail = tail.shape
    tok_rows, d_model = x_loc.shape
    group = n_tail * TAIL_CAP
    return pl.pallas_call(
        pick_tail_body,
        grid=(tok_rows // TILE,),
        in_specs=[SMEM, pl.BlockSpec((LANES, TILE), lambda i: (0, i)), ANY],
        out_specs=[pl.BlockSpec((group, d_model), lambda i: (0, 0))] * n_pos,
        scratch_shapes=[pltpu.VMEM((tok_rows, d_model), BF16), pltpu.SemaphoreType.DMA((tok_rows // TILE,))],
        out_shape=[jax.ShapeDtypeStruct((group, d_model), BF16)] * n_pos,
        compiler_params=params(1),
        cost_estimate=cost(2 * n_pos * group * tok_rows * d_model, 2 * tok_rows * d_model),
        name="pick_tail",
    )(tail, slot_t, x_loc)


def ffn_body(n_local, r_ref, src_ref, used_ref, *refs):
    n_src = 1 + MOVES
    own, (pg, pu, pd) = refs[: 3 * n_src], refs[3 * n_src : 3 * n_src + 3]
    refs = refs[3 * n_src + 3 :]
    n_rows = used_ref.shape[1]
    rows, outs, token = refs[:n_rows], refs[n_rows : 2 * n_rows], refs[2 * n_rows]
    x_buf, w_in, w_out, o_buf, x_sem, w_sem, o_sem = refs[2 * n_rows + 1 :]
    half, ffn = pg.shape
    q = lax.axis_index("data")
    r = r_ref[0]
    src = src_ref[r]
    token[0] = 0

    def load(place, parts, first):
        at = pl.ds(pl.multiple_of(place * half, half), half)
        places = (w_in.at[at, pl.ds(0, ffn)], w_in.at[at, pl.ds(ffn, ffn)], w_out.at[:, at])
        return [pltpu.make_async_copy(part, dst, w_sem.at[first + i]) for i, (part, dst) in enumerate(zip(parts, places))]

    row_loads = [pltpu.make_async_copy(rows[i], x_buf.at[i], x_sem.at[i]) for i in range(n_rows)]
    row_loads[0].start()
    theirs = load(1 - q, (pg, pu, pd), 3)
    for copy in theirs[:2]:
        copy.start()
    for s in range(n_src):
        @pl.when(jnp.maximum(src - n_local + 1, 0) == s)
        def _():
            parts = own[3 * s : 3 * s + 3]
            for copy in load(q, [part.at[jnp.minimum(src, n_local - 1)] for part in parts] if s == 0 else parts, 0):
                copy.start()
    theirs[2].start()
    for copy in row_loads[1:]:
        copy.start()
    ours = load(q, (pg, pu, pd), 0)
    for copy in row_loads + ours + theirs:
        copy.wait()

    part = LIGHT
    n_part = x_buf.shape[1] // part

    @pl.loop(0, n_rows)
    def _(i):
        @pl.loop(0, n_part)
        def _(j):
            at = pl.ds(pl.multiple_of(j * part, part), part)

            @pl.when(used_ref[r, i] > j * part)
            def _():
                act = jnp.dot(x_buf[i, at], w_in[...], preferred_element_type=F32)
                gate_act, up_act = act[:, :ffn], act[:, ffn:]
                hidden = (jax.nn.silu(gate_act) * up_act).astype(BF16)
                o_buf[i, at] = jnp.dot(hidden, w_out[...], preferred_element_type=F32).astype(BF16)

            @pl.when(used_ref[r, i] <= j * part)
            def _():
                o_buf[i, at] = jnp.zeros((part, o_buf.shape[2]), BF16)

        for s in range(n_rows):
            @pl.when(i == s)
            def _():
                pltpu.make_async_copy(o_buf.at[s], outs[s], o_sem.at[s]).start()

    for s in range(n_rows):
        pltpu.make_async_copy(o_buf.at[s], outs[s], o_sem.at[s]).wait()


def expert_ffn(r, sources, used, weights, extras, peer, rows):
    capacity, d_model = rows[0].shape
    n_local, half, ffn = weights[0].shape
    n_rows = len(rows)
    own = list(weights) + [part for extra in extras for part in extra]
    out = pl.pallas_call(
        functools.partial(ffn_body, n_local),
        in_specs=[SMEM] * 3 + [ANY] * (len(own) + 3 + n_rows),
        out_specs=[ANY] * n_rows + [SMEM],
        out_shape=[jax.ShapeDtypeStruct((capacity, d_model), BF16)] * n_rows + [TOKEN],
        scratch_shapes=[
            pltpu.VMEM((n_rows, capacity, d_model), BF16),
            pltpu.VMEM((2 * half, 2 * ffn), BF16),
            pltpu.VMEM((ffn, d_model), BF16),
            pltpu.VMEM((n_rows, capacity, d_model), BF16),
            pltpu.SemaphoreType.DMA((n_rows,)),
            pltpu.SemaphoreType.DMA((6,)),
            pltpu.SemaphoreType.DMA((n_rows,)),
        ],
        compiler_params=params(),
        cost_estimate=cost(6 * n_rows * capacity * d_model * ffn, 6 * d_model * ffn),
        name="ffn",
    )(r, sources, used, *own, *peer, *rows)
    return tuple(out[:n_rows]), out[n_rows]


def choose(ids, width):
    shape = (LANES, len(ids) * width)
    group = lax.broadcasted_iota(I32, shape, 1) // width
    wanted = jnp.full(shape, NO_EXPERT, I32)
    for i, e in enumerate(ids):
        wanted = jnp.where(group == i, e, wanted)
    return jnp.where(lax.broadcasted_iota(I32, shape, 0) == wanted, 1.0, 0.0).astype(BF16)


def chosen(pieces_ref, select):
    stacked = jnp.concatenate([pieces_ref[:, i * LANES : (i + 1) * LANES] for i in range(5)], axis=0)
    picked = jnp.dot(stacked, select, preferred_element_type=F32)
    high, low, *gates = [picked[i * TILE : (i + 1) * TILE] for i in range(5)]
    return 16.0 * high + low, gates


def weigh(hot, gates):
    return [jnp.where(hot, gate, 0.0).astype(BF16) for gate in gates]


def add_rows(out_ref, base_ref, terms):
    @pl.loop(0, out_ref.shape[1] // MIX_STRIP)
    def _(n):
        at = pl.ds(pl.multiple_of(n * MIX_STRIP, MIX_STRIP), MIX_STRIP)
        strip = base_ref[:, at]
        for weights, rows in terms:
            part = rows(at)
            strip = strip + sum(jnp.dot(weight, part, preferred_element_type=F32) for weight in weights)
        out_ref[:, at] = strip.astype(out_ref.dtype)


def mix_body(n_sets, has_tail, r_ref, tab_ref, start_ref, pieces_ref, acc_hbm, *refs):
    tails, refs = (refs[:2], refs[2:]) if has_tail else ((), refs)
    n_pos = tab_ref.shape[1]
    n_groups = n_sets * n_pos
    rows, (out_ref, token, total, select, sem, acc_buf, acc_sem, *held) = refs[:n_groups], refs[n_groups:]
    tile, n_tiles = pl.program_id(0), pl.num_programs(0)
    groups = [(held[g // n_pos].at[g % n_pos], tab_ref[r_ref[g // n_pos] + 1, g % n_pos]) for g in range(n_groups)]
    copies = [pltpu.make_async_copy(row, spot, sem.at[g]) for g, (row, (spot, _)) in enumerate(zip(rows, groups))]
    tail_ids = [tails[0][k, i] for k in range(tails[0].shape[0]) for i in range(tails[0].shape[1])] if has_tail else []
    n_main = n_groups * MIX_WINDOW

    def fetch(i):
        spot = lax.rem(i, AHEAD)
        return pltpu.make_async_copy(acc_hbm.at[pl.ds(pl.multiple_of(i * TILE, TILE), TILE)], acc_buf.at[spot], acc_sem.at[spot])

    @pl.when(tile == 0)
    def _():
        for copy in copies:
            copy.start()
        for i in range(AHEAD - 1):
            fetch(i).start()
        select[:, :n_main] = choose([e for _, e in groups], MIX_WINDOW)
        if has_tail:
            select[:, n_main:] = choose(tail_ids, TAIL_CAP)
        for copy in copies:
            copy.wait()

    @pl.when(tile + AHEAD - 1 < n_tiles)
    def _():
        fetch(tile + AHEAD - 1).start()

    fetch(tile).wait()
    acc_ref = acc_buf.at[lax.rem(tile, AHEAD)]
    token[0] = 0
    floors, counts = zip(*[windows(start_ref, tile, e, MIX_WINDOW) for _, e in groups])
    n_pass = functools.reduce(jnp.maximum, counts)
    column = lax.broadcasted_iota(I32, (1, n_main), 1)

    def term(w, slots, gates):
        firsts = [floor + w * MIX_WINDOW for floor in floors]
        bases = [pl.multiple_of(jnp.minimum(first, spot.shape[0] - MIX_WINDOW), 16) for first, (spot, _) in zip(firsts, groups)]
        first, place = jnp.zeros_like(column), column % MIX_WINDOW
        for g in range(n_groups):
            mine = column // MIX_WINDOW == g
            first = jnp.where(mine, firsts[g], first)
            place = jnp.where(mine, place + bases[g], place)
        hot = (slots == place.astype(F32)) & (slots >= first.astype(F32))
        return weigh(hot, gates), lambda at: jnp.concatenate([spot[pl.ds(base, MIX_WINDOW), at] for base, (spot, _) in zip(bases, groups)], axis=0)

    slots, gates = chosen(pieces_ref, select[...])
    terms = []
    if has_tail:
        tail_slots = slots[:, n_main:]
        place = lax.broadcasted_iota(I32, tail_slots.shape, 1) % TAIL_CAP
        terms.append((weigh(tail_slots == place.astype(F32), [gate[:, n_main:] for gate in gates]), lambda at: tails[1][:, at]))
    slots, gates = slots[:, :n_main], [gate[:, :n_main] for gate in gates]
    terms.append(term(0, slots, gates))

    @pl.when(n_pass <= 1)
    def _():
        add_rows(out_ref, acc_ref, terms)

    @pl.when(n_pass > 1)
    def _():
        add_rows(total, acc_ref, terms)

        @pl.loop(1, n_pass)
        def _(w):
            add_rows(total, total, [term(w, slots, gates)])

        out_ref[...] = total[...].astype(out_ref.dtype)


def mix(r, table, starts, pieces, sets, acc, out_dtype, tail=()):
    tok_rows, d_model = acc.shape
    rows = [row for group in sets for row in group]
    wide = pl.BlockSpec((TILE, d_model), lambda i: (i, 0))
    n_columns = len(rows) * MIX_WINDOW + (tail[1].shape[0] if tail else 0)
    return pl.pallas_call(
        functools.partial(mix_body, len(sets), bool(tail)),
        grid=(tok_rows // TILE,),
        in_specs=[
            SMEM,
            SMEM,
            SMEM,
            pl.BlockSpec((TILE, 5 * LANES), lambda i: (i, 0)),
            ANY,
            *([SMEM, pl.BlockSpec(tail[1].shape, lambda i: (0, 0))] if tail else []),
            *[ANY] * len(rows),
        ],
        out_specs=[wide, SMEM],
        scratch_shapes=[
            pltpu.VMEM((TILE, d_model), F32),
            pltpu.VMEM((LANES, n_columns), BF16),
            pltpu.SemaphoreType.DMA((len(rows),)),
            pltpu.VMEM((AHEAD, TILE, d_model), F32),
            pltpu.SemaphoreType.DMA((AHEAD,)),
            *[pltpu.VMEM((len(group), *group[0].shape), BF16) for group in sets],
        ],
        out_shape=[jax.ShapeDtypeStruct((tok_rows, d_model), out_dtype), TOKEN],
        input_output_aliases={4: 0} if acc.dtype == out_dtype else {},
        compiler_params=params(1),
        cost_estimate=cost(2 * len(rows) * tok_rows * WINDOW * d_model, 8 * tok_rows * d_model),
        name="mix",
    )(r, table, starts, pieces, acc, *tail, *rows)


def unset_body(*refs):
    pass


def unset(*shapes):
    return pl.pallas_call(unset_body, out_specs=[ANY] * len(shapes), out_shape=list(shapes), name="unset")()


def tail_in_body(idx_ref, mine_ref, peer_ref, wg_ref, wu_ref, mine_out, peer_out):
    rows, ffn = mine_ref.shape[1], wg_ref.shape[2]
    x = jnp.concatenate([mine_ref[0], peer_ref[0]], axis=0)
    for w_ref, first in ((wg_ref, 0), (wu_ref, ffn)):
        part = jnp.dot(x, w_ref[0], preferred_element_type=F32)
        mine_out[0, :, first : first + ffn] = part[:rows]
        peer_out[0, :, first : first + ffn] = part[rows:]


def tail_in(idx, mine, peer, w_gate, w_up):
    n_tail, rows, half = mine.shape
    ffn = w_gate.shape[2]
    weight = pl.BlockSpec((1, half, ffn), lambda i, idx: (idx[i], 0, 0))
    x_spec = pl.BlockSpec((1, rows, half), lambda i, idx: (i, 0, 0))
    return pl.pallas_call(
        tail_in_body,
        grid_spec=pltpu.PrefetchScalarGridSpec(
            num_scalar_prefetch=1,
            grid=(n_tail,),
            in_specs=[x_spec, x_spec, weight, weight],
            out_specs=[pl.BlockSpec((1, rows, 2 * ffn), lambda i, idx: (i, 0, 0))] * 2,
        ),
        out_shape=[jax.ShapeDtypeStruct((n_tail, rows, 2 * ffn), F32)] * 2,
        compiler_params=params(1),
        cost_estimate=cost(8 * n_tail * rows * half * ffn, 4 * n_tail * half * ffn),
        name="tail_in",
    )(idx, mine, peer, w_gate, w_up)


def tail_out_body(idx_ref, mine_ref, peer_ref, wd_ref, mine_out, peer_out):
    rows = mine_ref.shape[1]
    out = jnp.dot(jnp.concatenate([mine_ref[0], peer_ref[0]], axis=0), wd_ref[0], preferred_element_type=F32).astype(BF16)
    mine_out[0] = out[:rows]
    peer_out[0] = out[rows:]


def tail_out(idx, mine, peer, w_down):
    n_tail, rows, ffn = mine.shape
    half = w_down.shape[2]
    h_spec = pl.BlockSpec((1, rows, ffn), lambda i, idx: (i, 0, 0))
    return pl.pallas_call(
        tail_out_body,
        grid_spec=pltpu.PrefetchScalarGridSpec(
            num_scalar_prefetch=1,
            grid=(n_tail,),
            in_specs=[h_spec, h_spec, pl.BlockSpec((1, ffn, half), lambda i, idx: (idx[i], 0, 0))],
            out_specs=[pl.BlockSpec((1, rows, half), lambda i, idx: (i, 0, 0))] * 2,
        ),
        out_shape=[jax.ShapeDtypeStruct((n_tail, rows, half), BF16)] * 2,
        compiler_params=params(1),
        cost_estimate=cost(4 * n_tail * rows * half * ffn, 2 * n_tail * half * ffn),
        name="tail_out",
    )(idx, mine, peer, w_down)


def plan(counts, n_group):
    load = jnp.max(counts, axis=0).reshape(n_group, -1)
    n_local = load.shape[1]
    ids = jnp.arange(n_local, dtype=I32)
    ahead = (load[:, None, :] > load[:, :, None]) | ((load[:, None, :] == load[:, :, None]) & (ids[None, None, :] < ids[None, :, None]))
    rank = jnp.sum(ahead.astype(I32), axis=2)
    active = jnp.sum((load > 0).astype(I32), axis=1)
    tail = jnp.minimum(jnp.sum(((load > 0) & (load <= TAIL_CAP)).astype(I32), axis=1), TAIL)
    full = active - tail
    position = jnp.arange(n_group, dtype=I32)
    per_chip = jnp.max(jnp.sum(full.reshape(-1, 2), axis=1))
    least = (per_chip + 1) // 2
    limit = jnp.where(least >= MOVES + 2, MOVES, 0)
    n_round = jnp.maximum(jnp.maximum(least, jnp.max(full) - limit), 1)
    half = ((per_chip == 2 * n_round - 1) & (jnp.max(full * (position % 2)) - limit < n_round)).astype(I32)
    skip = half * (position % 2)
    give = jnp.clip(full - (n_round - skip), 0, limit)
    keep = full - give
    partner_keep = keep.reshape(-1, 2)[:, ::-1].reshape(-1)
    position = position[:, None]
    kept = rank < keep[:, None]
    in_round = rank < full[:, None]
    to = jnp.where(kept, position, position ^ 1)
    at = jnp.where(kept, rank + skip[:, None], jnp.maximum(partner_keep[:, None] + half * (1 - position % 2), 2) + rank - keep[:, None])
    source = jnp.where(kept, ids[None, :], n_local + rank - keep[:, None])
    tail_at = jnp.where((rank >= full[:, None]) & (rank < active[:, None]), rank - full[:, None], -1)
    n_slots = n_local + MOVES + 2
    flat = lambda a: jnp.broadcast_to(a, load.shape).reshape(-1)
    expert = jnp.arange(load.size, dtype=I32)
    rounds = jnp.arange(n_slots, dtype=I32)
    hit = (flat(to)[None, None, :] == position[:, :, None]) & (flat(at)[None, None, :] == rounds[None, :, None]) & flat(in_round)[None, None, :]
    table = jnp.max(jnp.where(hit, (expert + LANES * flat(source))[None, None, :], -1), axis=2)
    experts = jnp.where(table < 0, NO_EXPERT, table % LANES)
    sources = jnp.where(table < 0, 0, table // LANES)
    steps = jnp.arange(max(TAIL, MOVES), dtype=I32)
    tail_hit = tail_at[:, None, :] == steps[None, :TAIL, None]
    tails = jnp.max(jnp.where(tail_hit, ids[None, None, :], -1), axis=2)
    move_hit = (rank - keep[:, None])[:, None, :] == steps[None, :MOVES, None]
    moves = jnp.max(jnp.where(move_hit, ids[None, None, :], 0), axis=2)
    last_load = jnp.max(jnp.where((at == n_round - 1) & in_round, load, 0))
    return experts, sources, tails, moves, n_round, half, last_load


def solution(mesh):
    n_group, n_data = mesh.shape["expert"], mesh.shape["data"]
    assert n_group == 4 and n_data == 2
    tok_spec = P(("rep", "expert", "data"), None)
    wide_spec = P("expert", "data", None)
    down_spec = P("expert", None, "data")
    swap = [(0, 1), (1, 0)]

    def across(value, k):
        return lax.ppermute(value, "expert", [(p, p ^ k) for p in range(n_group)])

    def spread(groups):
        return (groups[0],) + tuple(across(groups[k], k) for k in range(1, n_group))

    def swapped(parts):
        return tuple(lax.ppermute(part, "data", swap) for part in parts)

    def device_body(x_loc, idx_loc, gate_loc, wg_loc, wu_loc, wd_loc):
        tok_rows, d_model = x_loc.shape
        top_k = idx_loc.shape[1]
        n_local = wg_loc.shape[0]
        n_exp = n_local * n_group
        capacity = capacity_rows(tok_rows, top_k, n_exp)
        me, q = lax.axis_index("expert"), lax.axis_index("data")
        weights = (wg_loc, wu_loc, wd_loc)
        pieces, slot_t, tile_starts, count = route(idx_loc.T, gate_loc.T, capacity)
        starts = jnp.concatenate([tile_starts[:, 0], count[:1]], axis=0)
        counts = lax.all_gather(count[0, :n_exp], ("expert", "data"))
        experts, sources, tails, moves, n_round, half_first, last_load = plan(counts, n_group)
        mine = me ^ jnp.arange(n_group, dtype=I32)
        table = jnp.concatenate([jnp.full((1, n_group), NO_EXPERT, I32), experts[mine].T], axis=0)
        my_sources = sources[me]
        my_hot = (experts[me][:, None] == jnp.arange(n_exp, dtype=I32)[None, :]).astype(I32)
        my_counts = counts.reshape(n_group, n_data, n_exp)[mine, q]
        used = jnp.sum(my_hot[:, None, :] * my_counts[None, :, :], axis=2)
        tail_local = jnp.maximum(tails[me], 0)
        tail_global = jnp.where(tails < 0, NO_EXPERT, tails + n_local * jnp.arange(n_group, dtype=I32)[:, None])[mine]

        def slices(e, source=None):
            return tuple(lax.dynamic_index_in_dim(w, e, axis=0, keepdims=False) for w in source or weights)

        def outgoing(r, extras):
            s = my_sources[r]
            kind = jnp.maximum(s - n_local + 1, 0)
            return lax.switch(kind, [lambda: slices(jnp.minimum(s, n_local - 1))] + [lambda i=i: extras[i] for i in range(MOVES)])

        half = d_model // n_data

        def one_round(r, carry, extras, first=False):
            token, peer, rows, back, send, acc = carry
            peer_next = swapped(send)
            *picked, token = pick(r + 1 + token, table, starts, slot_t, x_loc, capacity)
            rows_next = spread(picked)
            out_rows, token = expert_ffn(r + token, my_sources, used, weights, extras, peer, rows)
            back_next = spread(out_rows)
            send_next, token = lax.optimization_barrier((outgoing(r[0] + 2 + token[0], extras), token))
            if not first:
                acc, token = mix(r - 1 + token, table, starts, pieces, [back], acc, F32)
            return token, peer_next, rows_next, back_next, send_next, acc

        def front(i):
            only = (0, 2) if i % 2 else range(n_group)
            pairs = [(s * n_group + p, (1 - s) * n_group + p) for p in only for s in range(n_data)]
            peer = tuple(lax.ppermute(part, ("data", "expert"), pairs) for part in slices(first_sources[0]))
            tail_picked, token = lax.optimization_barrier((tuple(pick_tail(tail_global, slot_t, x_loc)), jnp.zeros((1,), I32)))
            tail_rows = spread(tail_picked)
            *picked, token = pick(token, table, starts, slot_t, x_loc, capacity)
            rows = (picked[0],) + tuple(lax.ppermute(picked[k], "expert", [(p ^ k, p) for p in only]) for k in range(1, n_group))
            later, token = lax.optimization_barrier((weights, token))
            moved, token = lax.optimization_barrier(([slices(move + token[0], later) for move in my_moves], token))
            extras = tuple(tuple(across(part, 1) for part in parts) for parts in moved)
            later, token = lax.optimization_barrier((weights, token))
            send, token = lax.optimization_barrier((slices(first_sources[1] + token[0], later), token))
            tail_x = jnp.stack([group.reshape(TAIL, TAIL_CAP, d_model) for group in tail_rows], axis=1).reshape(TAIL, n_group * TAIL_CAP, d_model)
            tail_mine = lax.dynamic_slice_in_dim(tail_x, q * half, half, axis=2)
            tail_half, token = lax.optimization_barrier((lax.dynamic_slice_in_dim(tail_x, (1 - q) * half, half, axis=2), token))
            tail_peer = lax.ppermute(tail_half, "data", swap)
            x_later, token = lax.optimization_barrier((x_loc, token))
            acc, token = lax.optimization_barrier((x_later.astype(F32), token))
            blank = tuple(unset(*[jax.ShapeDtypeStruct((capacity, d_model), BF16)] * n_group))
            carry = (token, peer, rows, blank, send, acc)
            if i >= 2:
                carry = one_round(jnp.zeros((1,), I32), carry, extras, first=True)
            return carry, extras, tail_mine, tail_peer

        first_sources = [my_sources[0], my_sources[1]]
        my_moves = [moves[me, m] for m in range(MOVES)]
        odd = (n_round - 1) % 2
        carry, extras, tail_mine, tail_peer = lax.switch(2 * odd + half_first, [functools.partial(front, i) for i in range(4)])

        def two_rounds(i, c):
            r = jnp.full((1,), odd + 2 * i, I32)
            return one_round(r + 1, one_round(r, c, extras), extras)

        token, peer, rows, back, _, acc = lax.fori_loop(0, (n_round - 1) // 2, two_rounds, carry)
        last = jnp.full((1,), n_round - 1, I32)
        ffn = wg_loc.shape[2]

        partial, partial_peer = tail_in(tail_local + token, tail_mine, tail_peer, wg_loc, wu_loc)
        (partial, partial_peer), token = lax.optimization_barrier(((partial, partial_peer), token))
        partial_sum = partial + lax.ppermute(partial_peer, "data", swap)
        out_last, token = expert_ffn(last + token, my_sources, used, weights, extras, peer, rows)

        def diagonal(value, k):
            pairs = [(s * n_group + p, (1 - s) * n_group + (p ^ k)) for p in range(n_group) for s in range(n_data)]
            return lax.ppermute(value, ("data", "expert"), pairs)

        def finish(keep):
            def run():
                back_last = spread([group[:keep] for group in out_last])
                tail_h = (jax.nn.silu(partial_sum[..., :ffn]) * partial_sum[..., ffn:]).astype(BF16)
                tail_h_peer = lax.ppermute(tail_h, "data", swap)
                if keep == LIGHT:
                    acc_late, go = acc, token
                else:
                    acc_late, go = mix(last - 1 + token, table, starts, pieces, [back], acc, F32)
                mine, theirs = tail_out(tail_local + go, tail_h, tail_h_peer, wd_loc)
                mine, theirs = (o.reshape(TAIL, n_group, TAIL_CAP, half) for o in (mine, theirs))
                tail_halves = []
                for k in range(n_group):
                    near, far = mine[:, k].reshape(TAIL * TAIL_CAP, half), theirs[:, k].reshape(TAIL * TAIL_CAP, half)
                    tail_halves.append((across(near, k) if k else near, diagonal(far, k)))
                near, far = (jnp.concatenate(parts, axis=0) for parts in zip(*tail_halves))
                tail_rows = jnp.where(q == 0, jnp.concatenate([near, far], axis=1), jnp.concatenate([far, near], axis=1))
                tail = (tail_global, tail_rows)
                if keep == LIGHT:
                    return mix(jnp.concatenate([last - 1 + go, last]), table, starts, pieces, [back, back_last], acc_late, BF16, tail)[0]
                return mix(last + go, table, starts, pieces, [back_last], acc_late, BF16, tail)[0]

            return run

        return lax.cond(last_load <= LIGHT, finish(LIGHT), finish(capacity))

    return jax.shard_map(device_body, mesh=mesh, in_specs=(tok_spec, tok_spec, tok_spec, wide_spec, wide_spec, down_spec), out_specs=tok_spec, check_vma=False)
```

```python
import functools

import jax
import jax.numpy as jnp
from jax import lax
from jax.experimental import pallas as pl
from jax.experimental.pallas import tpu as pltpu
from jax.sharding import PartitionSpec as P


LANES = 128
NO_EXPERT = LANES - 1
TILE = 256
WINDOW = 128
MOVES = 2
LAST_PART = 160
LIGHT = 320
TAIL, TAIL_CAP = 3, 16
BF16, F32, I32 = jnp.bfloat16, jnp.float32, jnp.int32
ANY = pl.BlockSpec(memory_space=pl.ANY)
SMEM = pl.BlockSpec(memory_space=pltpu.SMEM)
VMEM_LIMIT = 62 * 1024 * 1024
TOKEN = jax.ShapeDtypeStruct((1,), I32)


def capacity_rows(tok_rows, top_k, n_exp):
    return max(8, ((5 * top_k * tok_rows) // (4 * n_exp) + 7) // 8 * 8)


def params(n_axes=0):
    return pltpu.CompilerParams(dimension_semantics=("arbitrary",) * n_axes if n_axes else None, vmem_limit_bytes=VMEM_LIMIT)


def cost(flops, bytes_accessed):
    return pl.CostEstimate(flops=flops, bytes_accessed=bytes_accessed, transcendentals=0)


def route_body(capacity, ids_ref, gate_ref, slot_ref, slot_t_ref, gate_te_ref, start_ref, count_ref, seen):
    @pl.when(pl.program_id(0) == 0)
    def _():
        seen[...] = jnp.zeros_like(seen)

    top_k, tile = ids_ref.shape
    expert = lax.broadcasted_iota(I32, (LANES, tile), 0)
    mask = jnp.zeros((LANES, tile), F32)
    gate_t = jnp.zeros((LANES, tile), F32)
    for j in range(top_k):
        hit = ids_ref[j : j + 1, :] == expert
        mask = jnp.where(hit, 1.0, mask)
        gate_t = jnp.where(hit, gate_ref[j : j + 1, :], gate_t)
    before = lax.broadcasted_iota(I32, (tile, tile), 0) < lax.broadcasted_iota(I32, (tile, tile), 1)
    earlier = jnp.dot(mask.astype(BF16), jnp.where(before, 1.0, 0.0).astype(BF16), preferred_element_type=F32) + seen[:, 0:1]
    slot = jnp.where((mask > 0.0) & (earlier < capacity), earlier, -1.0)
    slot_t_ref[...] = slot.astype(I32)
    slot_ref[...] = slot.T.astype(I32)
    gate_te_ref[...] = gate_t.T
    start_ref[0] = jnp.minimum(seen[...].T[:8], capacity).astype(I32)
    seen[...] = seen[...] + jnp.sum(mask, axis=1, keepdims=True)
    count_ref[...] = jnp.minimum(seen[...].T[:8], capacity).astype(I32)


def route(ids_t, gate_t, capacity):
    top_k, tok_rows = ids_t.shape
    n_tiles = tok_rows // TILE
    col = pl.BlockSpec((TILE, LANES), lambda i: (i, 0))
    return pl.pallas_call(
        functools.partial(route_body, capacity),
        grid=(n_tiles,),
        in_specs=[pl.BlockSpec((top_k, TILE), lambda i: (0, i))] * 2,
        out_specs=[
            col,
            pl.BlockSpec((LANES, TILE), lambda i: (0, i)),
            col,
            pl.BlockSpec((1, 8, LANES), lambda i: (i, 0, 0)),
            pl.BlockSpec((8, LANES), lambda i: (0, 0)),
        ],
        out_shape=[
            jax.ShapeDtypeStruct((tok_rows, LANES), I32),
            jax.ShapeDtypeStruct((LANES, tok_rows), I32),
            jax.ShapeDtypeStruct((tok_rows, LANES), F32),
            jax.ShapeDtypeStruct((n_tiles, 8, LANES), I32),
            jax.ShapeDtypeStruct((8, LANES), I32),
        ],
        scratch_shapes=[pltpu.VMEM((LANES, LANES), F32)],
        compiler_params=params(1),
        name="route",
    )(ids_t, gate_t)


def windows(start_ref, tile, e, capacity, step):
    lo, hi = start_ref[tile, e], start_ref[tile + 1, e]
    floor = lo // 16 * 16
    n_win = jnp.where(hi > lo, (hi - floor + WINDOW - 1) // WINDOW, 0)

    @pl.loop(0, n_win)
    def _(w):
        first = floor + w * WINDOW
        step(first, pl.multiple_of(jnp.minimum(first, capacity - WINDOW), 16))


def pick_body(r_ref, tab_ref, start_ref, slot_t_ref, x_ref, *refs):
    outs, token = refs[:-1], refs[-1]
    tile = pl.program_id(0)
    token[0] = 0

    @pl.when(tile == 0)
    def _():
        for out in outs:
            out[...] = jnp.zeros_like(out)

    for k, out in enumerate(outs):
        e = tab_ref[r_ref[0] + 1, k]

        def step(first, base, out=out, e=e):
            slots = slot_t_ref[pl.ds(e, 1), :]
            row = lax.broadcasted_iota(I32, (WINDOW, TILE), 0) + base
            hot = jnp.where((row == slots) & (slots >= first), 1.0, 0.0).astype(BF16)
            out[pl.ds(base, WINDOW), :] += jnp.dot(hot, x_ref[...], preferred_element_type=F32).astype(BF16)

        windows(start_ref, tile, e, out.shape[0], step)


def pick(r, table, starts, slot_t, x_loc, capacity):
    n_pick = table.shape[1]
    tok_rows, d_model = x_loc.shape
    return pl.pallas_call(
        pick_body,
        grid=(tok_rows // TILE,),
        in_specs=[
            SMEM,
            SMEM,
            SMEM,
            pl.BlockSpec((LANES, TILE), lambda i: (0, i)),
            pl.BlockSpec((TILE, d_model), lambda i: (i, 0)),
        ],
        out_specs=[pl.BlockSpec((capacity, d_model), lambda i: (0, 0))] * n_pick + [SMEM],
        out_shape=[jax.ShapeDtypeStruct((capacity, d_model), BF16)] * n_pick + [TOKEN],
        compiler_params=params(1),
        cost_estimate=cost(2 * n_pick * capacity * TILE * d_model, 2 * tok_rows * d_model),
        name="pick",
    )(r, table, starts, slot_t, x_loc)


def pick_tail_body(tail_ref, slot_t_ref, x_ref, *outs):
    tile = pl.program_id(0)
    n_tail = tail_ref.shape[1]
    group = n_tail * TAIL_CAP
    hots = []
    for k in range(len(outs)):
        for i in range(n_tail):
            row = lax.broadcasted_iota(I32, (TAIL_CAP, x_ref.shape[0]), 0)
            hots.append(jnp.where(row == slot_t_ref[pl.ds(tail_ref[k, i], 1), :], 1.0, 0.0).astype(BF16))
    picked = jnp.dot(jnp.concatenate(hots, axis=0), x_ref[...], preferred_element_type=F32).astype(BF16)

    @pl.when(tile == 0)
    def _():
        for out in outs:
            out[...] = jnp.zeros_like(out)

    for k, out in enumerate(outs):
        out[...] += picked[k * group : (k + 1) * group]


def pick_tail(tail, slot_t, x_loc):
    n_pos, n_tail = tail.shape
    tok_rows, d_model = x_loc.shape
    group = n_tail * TAIL_CAP
    return pl.pallas_call(
        pick_tail_body,
        grid=(tok_rows // TILE,),
        in_specs=[SMEM, pl.BlockSpec((LANES, TILE), lambda i: (0, i)), pl.BlockSpec((TILE, d_model), lambda i: (i, 0))],
        out_specs=[pl.BlockSpec((group, d_model), lambda i: (0, 0))] * n_pos,
        out_shape=[jax.ShapeDtypeStruct((group, d_model), BF16)] * n_pos,
        compiler_params=params(1),
        cost_estimate=cost(2 * n_pos * group * tok_rows * d_model, 2 * tok_rows * d_model),
        name="pick_tail",
    )(tail, slot_t, x_loc)


def ffn_body(n_local, r_ref, src_ref, used_ref, *refs):
    n_src = 1 + MOVES
    own, (pg, pu, pd) = refs[: 3 * n_src], refs[3 * n_src : 3 * n_src + 3]
    refs = refs[3 * n_src + 3 :]
    n_rows = used_ref.shape[1]
    rows, outs, token = refs[:n_rows], refs[n_rows : 2 * n_rows], refs[2 * n_rows]
    x_buf, w_in, w_out, o_buf, x_sem, w_sem, o_sem = refs[2 * n_rows + 1 :]
    half, ffn = pg.shape
    q = lax.axis_index("data")
    r = r_ref[0]
    src = src_ref[r]
    token[0] = 0

    def load(place, parts, first):
        at = pl.ds(pl.multiple_of(place * half, half), half)
        places = (w_in.at[at, pl.ds(0, ffn)], w_in.at[at, pl.ds(ffn, ffn)], w_out.at[:, at])
        return [pltpu.make_async_copy(part, dst, w_sem.at[first + i]) for i, (part, dst) in enumerate(zip(parts, places))]

    row_loads = [pltpu.make_async_copy(rows[i], x_buf.at[i], x_sem.at[i]) for i in range(n_rows)]
    row_loads[0].start()
    theirs = load(1 - q, (pg, pu, pd), 3)
    for copy in theirs[:2]:
        copy.start()
    for s in range(n_src):
        @pl.when(jnp.maximum(src - n_local + 1, 0) == s)
        def _():
            parts = own[3 * s : 3 * s + 3]
            for copy in load(q, [part.at[jnp.minimum(src, n_local - 1)] for part in parts] if s == 0 else parts, 0):
                copy.start()
    theirs[2].start()
    for copy in row_loads[1:]:
        copy.start()
    ours = load(q, (pg, pu, pd), 0)
    for copy in row_loads + ours + theirs:
        copy.wait()

    n_part = 2
    part = x_buf.shape[1] // n_part

    @pl.loop(0, n_rows)
    def _(i):
        @pl.loop(0, n_part)
        def _(j):
            at = pl.ds(pl.multiple_of(j * part, part), part)

            @pl.when(used_ref[r, i] > j * part)
            def _():
                act = jnp.dot(x_buf[i, at], w_in[...], preferred_element_type=F32)
                gate_act, up_act = act[:, :ffn], act[:, ffn:]
                hidden = (jax.nn.silu(gate_act) * up_act).astype(BF16)
                o_buf[i, at] = jnp.dot(hidden, w_out[...], preferred_element_type=F32).astype(BF16)

            @pl.when(used_ref[r, i] <= j * part)
            def _():
                o_buf[i, at] = jnp.zeros((part, o_buf.shape[2]), BF16)

        for s in range(n_rows):
            @pl.when(i == s)
            def _():
                pltpu.make_async_copy(o_buf.at[s], outs[s], o_sem.at[s]).start()

    for s in range(n_rows):
        pltpu.make_async_copy(o_buf.at[s], outs[s], o_sem.at[s]).wait()


def expert_ffn(r, sources, used, weights, extras, peer, rows):
    capacity, d_model = rows[0].shape
    n_local, half, ffn = weights[0].shape
    n_rows = len(rows)
    own = list(weights) + [part for extra in extras for part in extra]
    out = pl.pallas_call(
        functools.partial(ffn_body, n_local),
        in_specs=[SMEM] * 3 + [ANY] * (len(own) + 3 + n_rows),
        out_specs=[ANY] * n_rows + [SMEM],
        out_shape=[jax.ShapeDtypeStruct((capacity, d_model), BF16)] * n_rows + [TOKEN],
        scratch_shapes=[
            pltpu.VMEM((n_rows, capacity, d_model), BF16),
            pltpu.VMEM((2 * half, 2 * ffn), BF16),
            pltpu.VMEM((ffn, d_model), BF16),
            pltpu.VMEM((n_rows, capacity, d_model), BF16),
            pltpu.SemaphoreType.DMA((n_rows,)),
            pltpu.SemaphoreType.DMA((6,)),
            pltpu.SemaphoreType.DMA((n_rows,)),
        ],
        compiler_params=params(),
        cost_estimate=cost(6 * n_rows * capacity * d_model * ffn, 6 * d_model * ffn),
        name="ffn",
    )(r, sources, used, *own, *peer, *rows)
    return tuple(out[:n_rows]), out[n_rows]


def choose_source(src, n_local, sources, act):
    for s, parts in enumerate(sources):
        @pl.when(jnp.maximum(src - n_local + 1, 0) == s)
        def _():
            act([part.at[jnp.minimum(src, n_local - 1)] for part in parts] if s == 0 else parts)


def ffn_up_body(n_local, r_ref, src_ref, used_ref, *refs):
    n_src, n_rows = 1 + MOVES, used_ref.shape[1]
    own, refs = refs[: 2 * n_src], refs[2 * n_src :]
    pg, pu, *refs = refs
    rows, (h_out, token, x_buf, w_in, h_buf, x_sem, w_sem, h_sem) = refs[:n_rows], refs[n_rows:]
    half, ffn = pg.shape
    q = lax.axis_index("data")
    r = r_ref[0]
    token[0] = 0

    def load(place, parts, first):
        at = pl.ds(pl.multiple_of(place * half, half), half)
        return [pltpu.make_async_copy(part, w_in.at[at, pl.ds(i * ffn, ffn)], w_sem.at[first + i]) for i, part in enumerate(parts)]

    def start_all(parts):
        for copy in load(q, parts, 0):
            copy.start()

    row_loads = [pltpu.make_async_copy(rows[i], x_buf.at[i], x_sem.at[i]) for i in range(n_rows)]
    for copy in row_loads + load(1 - q, (pg, pu), 2):
        copy.start()
    choose_source(src_ref[r], n_local, [own[2 * s : 2 * s + 2] for s in range(n_src)], start_all)
    for copy in row_loads + load(q, (pg, pu), 0) + load(1 - q, (pg, pu), 2):
        copy.wait()

    part = LAST_PART

    @pl.loop(0, n_rows)
    def _(i):
        @pl.loop(0, x_buf.shape[1] // part)
        def _(j):
            at = pl.ds(pl.multiple_of(j * part, part), part)

            @pl.when(used_ref[r, i] > j * part)
            def _():
                act = jnp.dot(x_buf[i, at], w_in[...], preferred_element_type=F32)
                h_buf[i, at] = (jax.nn.silu(act[:, :ffn]) * act[:, ffn:]).astype(BF16)

            @pl.when(used_ref[r, i] <= j * part)
            def _():
                h_buf[i, at] = jnp.zeros((part, ffn), BF16)

        pltpu.make_async_copy(h_buf.at[i], h_out.at[i], h_sem.at[i]).start()

    for i in range(n_rows):
        pltpu.make_async_copy(h_buf.at[i], h_out.at[i], h_sem.at[i]).wait()


def ffn_up(r, sources, used, weights, extras, peer, rows):
    capacity, d_model = rows[0].shape
    n_local, half, ffn = weights[0].shape
    n_rows = len(rows)
    own = list(weights[:2]) + [part for extra in extras for part in extra[:2]]
    return pl.pallas_call(
        functools.partial(ffn_up_body, n_local),
        in_specs=[SMEM] * 3 + [ANY] * (len(own) + 2 + n_rows),
        out_specs=[ANY, SMEM],
        out_shape=[jax.ShapeDtypeStruct((n_rows, capacity, ffn), BF16), TOKEN],
        scratch_shapes=[
            pltpu.VMEM((n_rows, capacity, d_model), BF16),
            pltpu.VMEM((2 * half, 2 * ffn), BF16),
            pltpu.VMEM((n_rows, capacity, ffn), BF16),
            pltpu.SemaphoreType.DMA((n_rows,)),
            pltpu.SemaphoreType.DMA((4,)),
            pltpu.SemaphoreType.DMA((n_rows,)),
        ],
        compiler_params=params(),
        cost_estimate=cost(4 * n_rows * capacity * d_model * ffn, 4 * d_model * ffn),
        name="ffn_up",
    )(r, sources, used, *own, *peer[:2], *rows)


def ffn_down_body(n_local, r_ref, src_ref, used_ref, *refs):
    n_src, n_rows = 1 + MOVES, used_ref.shape[1]
    own, refs = refs[:n_src], refs[n_src:]
    pd, h_in, *refs = refs
    outs, (token, h_buf, w_out, o_buf, h_sem, w_sem, o_sem) = refs[: 2 * n_rows], refs[2 * n_rows :]
    half = pd.shape[1]
    q = lax.axis_index("data")
    r = r_ref[0]
    token[0] = 0

    def load(place, part, i):
        return pltpu.make_async_copy(part, w_out.at[:, pl.ds(pl.multiple_of(place * half, half), half)], w_sem.at[i])

    def store(s):
        parts = (o_buf.at[s, pl.ds(0, LIGHT)], o_buf.at[s, pl.ds(LIGHT, o_buf.shape[1] - LIGHT)])
        return [pltpu.make_async_copy(part, outs[2 * s + i], o_sem.at[s, i]) for i, part in enumerate(parts)]

    h_load = pltpu.make_async_copy(h_in, h_buf, h_sem)
    h_load.start()
    load(1 - q, pd, 1).start()
    choose_source(src_ref[r], n_local, [own[s : s + 1] for s in range(n_src)], lambda parts: load(q, parts[0], 0).start())
    h_load.wait()
    load(q, pd, 0).wait()
    load(1 - q, pd, 1).wait()
    part = LAST_PART

    @pl.loop(0, n_rows)
    def _(i):
        @pl.loop(0, h_buf.shape[1] // part)
        def _(j):
            at = pl.ds(pl.multiple_of(j * part, part), part)

            @pl.when(used_ref[r, i] > j * part)
            def _():
                o_buf[i, at] = jnp.dot(h_buf[i, at], w_out[...], preferred_element_type=F32).astype(BF16)

            @pl.when(used_ref[r, i] <= j * part)
            def _():
                o_buf[i, at] = jnp.zeros((part, o_buf.shape[2]), BF16)

        for s in range(n_rows):
            @pl.when(i == s)
            def _():
                for copy in store(s):
                    copy.start()

    for s in range(n_rows):
        for copy in store(s):
            copy.wait()


def ffn_down(r, sources, used, weights, extras, peer, hidden):
    n_rows, capacity, ffn = hidden.shape
    n_local, _, half = weights[2].shape
    d_model = 2 * half
    own = [weights[2]] + [extra[2] for extra in extras]
    pieces = [jax.ShapeDtypeStruct((LIGHT, d_model), BF16), jax.ShapeDtypeStruct((capacity - LIGHT, d_model), BF16)]
    out = pl.pallas_call(
        functools.partial(ffn_down_body, n_local),
        in_specs=[SMEM] * 3 + [ANY] * (len(own) + 2),
        out_specs=[ANY] * (2 * n_rows) + [SMEM],
        out_shape=pieces * n_rows + [TOKEN],
        scratch_shapes=[
            pltpu.VMEM((n_rows, capacity, ffn), BF16),
            pltpu.VMEM((ffn, d_model), BF16),
            pltpu.VMEM((n_rows, capacity, d_model), BF16),
            pltpu.SemaphoreType.DMA,
            pltpu.SemaphoreType.DMA((2,)),
            pltpu.SemaphoreType.DMA((n_rows, 2)),
        ],
        compiler_params=params(),
        cost_estimate=cost(2 * n_rows * capacity * d_model * ffn, 2 * d_model * ffn),
        name="ffn_down",
    )(r, sources, used, *own, peer[2], hidden)
    return out[0 : 2 * n_rows : 2], out[1 : 2 * n_rows : 2], out[2 * n_rows]


def tail_sum(tail_ref, slot_ref, gate_ref, rows_ref, total):
    n_pos, n_tail = tail_ref.shape
    n_col = rows_ref.shape[0]
    row = lax.broadcasted_iota(I32, (LANES, n_col), 0)
    group = lax.broadcasted_iota(I32, (LANES, n_col), 1) // TAIL_CAP
    wanted = jnp.full((LANES, n_col), NO_EXPERT, I32)
    for k in range(n_pos):
        for i in range(n_tail):
            wanted = jnp.where(group == k * n_tail + i, tail_ref[k, i], wanted)
    select = jnp.where(row == wanted, 1.0, 0.0).astype(BF16)
    slots = jnp.dot(slot_ref[...].astype(F32).astype(BF16), select, preferred_element_type=F32)
    place = lax.broadcasted_iota(I32, (TILE, n_col), 1) % TAIL_CAP
    here = slots == place.astype(F32)
    rest = gate_ref[...]
    weights = []
    for _ in range(3):
        piece = rest.astype(BF16)
        rest = rest - piece.astype(F32)
        weights.append(jnp.where(here, jnp.dot(piece, select, preferred_element_type=F32), 0.0).astype(BF16))
    parts = jnp.dot(jnp.concatenate(weights, axis=0), rows_ref[...], preferred_element_type=F32)
    total[...] += parts[:TILE] + parts[TILE : 2 * TILE] + parts[2 * TILE :]


def mix_body(has_tail, r_ref, tab_ref, start_ref, slot_ref, gate_ref, *refs):
    n_rows = tab_ref.shape[1]
    if has_tail:
        firsts, others, refs = refs[:n_rows], refs[n_rows : 2 * n_rows], refs[2 * n_rows :]
        acc_ref, *tails, out_ref, token, total, held, sem = refs
        rows = [held.at[k] for k in range(n_rows)]
        copies = []
        for k in range(n_rows):
            for i, (part, spot) in enumerate(((firsts[k], pl.ds(0, LIGHT)), (others[k], pl.ds(LIGHT, others[k].shape[0])))):
                copies.append(pltpu.make_async_copy(part, held.at[k, spot], sem.at[k, i]))

        @pl.when(pl.program_id(0) == 0)
        def _():
            for copy in copies:
                copy.start()
            for copy in copies:
                copy.wait()
    else:
        rows, (acc_ref, out_ref, token, total) = refs[:n_rows], refs[n_rows:]
    tile = pl.program_id(0)
    token[0] = 0
    total[...] = acc_ref[...]
    if has_tail:
        tail_sum(tails[0], slot_ref, gate_ref, tails[1], total)
    lane = lax.broadcasted_iota(I32, (TILE, LANES), 1)
    for k in range(n_rows):
        e = tab_ref[r_ref[0] + 1, k]

        def step(first, base, k=k, e=e):
            here = lane == e
            slots = jnp.max(jnp.where(here, slot_ref[...], -1), axis=1, keepdims=True)
            gates = jnp.sum(jnp.where(here, gate_ref[...], 0.0), axis=1, keepdims=True)
            column = lax.broadcasted_iota(I32, (TILE, WINDOW), 1) + base
            hot = jnp.where((column == slots) & (slots >= first), 1.0, 0.0).astype(BF16)
            total[...] += gates * jnp.dot(hot, rows[k][pl.ds(base, WINDOW), :], preferred_element_type=F32)

        windows(start_ref, tile, e, rows[k].shape[0], step)
    out_ref[...] = total[...].astype(out_ref.dtype)


def mix(r, table, starts, slot, gate_te, rows, acc, out_dtype, tail=()):
    n_rows = table.shape[1]
    tok_rows, d_model = acc.shape
    col = pl.BlockSpec((TILE, LANES), lambda i: (i, 0))
    wide = pl.BlockSpec((TILE, d_model), lambda i: (i, 0))

    def held(value):
        return pl.BlockSpec(value.shape, lambda i: (0, 0), pipeline_mode=pl.Buffered(1))

    scratch = [pltpu.VMEM((TILE, d_model), F32)]
    if tail:
        capacity = rows[0].shape[0] + rows[n_rows].shape[0]
        scratch += [pltpu.VMEM((n_rows, capacity, d_model), BF16), pltpu.SemaphoreType.DMA((n_rows, 2))]
    return pl.pallas_call(
        functools.partial(mix_body, bool(tail)),
        grid=(tok_rows // TILE,),
        in_specs=[SMEM, SMEM, SMEM, col, col] + [ANY if tail else held(row) for row in rows] + [wide] + ([SMEM, held(tail[1])] if tail else []),
        out_specs=[wide, SMEM],
        out_shape=[jax.ShapeDtypeStruct((tok_rows, d_model), out_dtype), TOKEN],
        scratch_shapes=scratch,
        input_output_aliases={5 + n_rows: 0} if acc.dtype == out_dtype else {},
        compiler_params=params(1),
        cost_estimate=cost(2 * n_rows * tok_rows * WINDOW * d_model, 8 * tok_rows * d_model),
        name="mix",
    )(r, table, starts, slot, gate_te, *rows, acc, *tail)


def unset_body(*refs):
    pass


def unset(*shapes):
    return pl.pallas_call(unset_body, out_specs=[ANY] * len(shapes), out_shape=list(shapes), name="unset")()


def tail_in_body(idx_ref, mine_ref, peer_ref, wg_ref, wu_ref, mine_out, peer_out):
    rows, ffn = mine_ref.shape[1], wg_ref.shape[2]
    x = jnp.concatenate([mine_ref[0], peer_ref[0]], axis=0)
    for w_ref, first in ((wg_ref, 0), (wu_ref, ffn)):
        part = jnp.dot(x, w_ref[0], preferred_element_type=F32)
        mine_out[0, :, first : first + ffn] = part[:rows]
        peer_out[0, :, first : first + ffn] = part[rows:]


def tail_in(idx, mine, peer, w_gate, w_up):
    n_tail, rows, half = mine.shape
    ffn = w_gate.shape[2]
    weight = pl.BlockSpec((1, half, ffn), lambda i, idx: (idx[i], 0, 0))
    x_spec = pl.BlockSpec((1, rows, half), lambda i, idx: (i, 0, 0))
    return pl.pallas_call(
        tail_in_body,
        grid_spec=pltpu.PrefetchScalarGridSpec(
            num_scalar_prefetch=1,
            grid=(n_tail,),
            in_specs=[x_spec, x_spec, weight, weight],
            out_specs=[pl.BlockSpec((1, rows, 2 * ffn), lambda i, idx: (i, 0, 0))] * 2,
        ),
        out_shape=[jax.ShapeDtypeStruct((n_tail, rows, 2 * ffn), F32)] * 2,
        compiler_params=params(1),
        cost_estimate=cost(8 * n_tail * rows * half * ffn, 4 * n_tail * half * ffn),
        name="tail_in",
    )(idx, mine, peer, w_gate, w_up)


def tail_out_body(idx_ref, mine_ref, peer_ref, wd_ref, mine_out, peer_out):
    rows = mine_ref.shape[1]
    out = jnp.dot(jnp.concatenate([mine_ref[0], peer_ref[0]], axis=0), wd_ref[0], preferred_element_type=F32).astype(BF16)
    mine_out[0] = out[:rows]
    peer_out[0] = out[rows:]


def tail_out(idx, mine, peer, w_down):
    n_tail, rows, ffn = mine.shape
    half = w_down.shape[2]
    h_spec = pl.BlockSpec((1, rows, ffn), lambda i, idx: (i, 0, 0))
    return pl.pallas_call(
        tail_out_body,
        grid_spec=pltpu.PrefetchScalarGridSpec(
            num_scalar_prefetch=1,
            grid=(n_tail,),
            in_specs=[h_spec, h_spec, pl.BlockSpec((1, ffn, half), lambda i, idx: (idx[i], 0, 0))],
            out_specs=[pl.BlockSpec((1, rows, half), lambda i, idx: (i, 0, 0))] * 2,
        ),
        out_shape=[jax.ShapeDtypeStruct((n_tail, rows, half), BF16)] * 2,
        compiler_params=params(1),
        cost_estimate=cost(4 * n_tail * rows * half * ffn, 2 * n_tail * half * ffn),
        name="tail_out",
    )(idx, mine, peer, w_down)


def plan(counts, n_group):
    load = jnp.max(counts, axis=0).reshape(n_group, -1)
    n_local = load.shape[1]
    ids = jnp.arange(n_local, dtype=I32)
    ahead = (load[:, None, :] > load[:, :, None]) | ((load[:, None, :] == load[:, :, None]) & (ids[None, None, :] < ids[None, :, None]))
    rank = jnp.sum(ahead.astype(I32), axis=2)
    active = jnp.sum((load > 0).astype(I32), axis=1)
    tail = jnp.minimum(jnp.sum(((load > 0) & (load <= TAIL_CAP)).astype(I32), axis=1), TAIL)
    full = active - tail
    position = jnp.arange(n_group, dtype=I32)[:, None]
    least = (jnp.max(jnp.sum(full.reshape(-1, 2), axis=1)) + 1) // 2
    limit = jnp.where(least >= MOVES + 2, MOVES, 0)
    n_round = jnp.maximum(jnp.maximum(least, jnp.max(full) - limit), 2)
    give = jnp.clip(full - n_round, 0, limit)
    keep = full - give
    partner_keep = keep.reshape(-1, 2)[:, ::-1].reshape(-1)
    kept = rank < keep[:, None]
    in_round = rank < full[:, None]
    to = jnp.where(kept, position, position ^ 1)
    at = jnp.where(kept, rank, jnp.maximum(partner_keep[:, None], 2) + rank - keep[:, None])
    source = jnp.where(kept, ids[None, :], n_local + rank - keep[:, None])
    tail_at = jnp.where((rank >= full[:, None]) & (rank < active[:, None]), rank - full[:, None], -1)
    n_slots = n_local + MOVES + 2
    flat = lambda a: jnp.broadcast_to(a, load.shape).reshape(-1)
    expert = jnp.arange(load.size, dtype=I32)
    rounds = jnp.arange(n_slots, dtype=I32)
    hit = (flat(to)[None, None, :] == position[:, :, None]) & (flat(at)[None, None, :] == rounds[None, :, None]) & flat(in_round)[None, None, :]
    table = jnp.max(jnp.where(hit, (expert + LANES * flat(source))[None, None, :], -1), axis=2)
    experts = jnp.where(table < 0, NO_EXPERT, table % LANES)
    sources = jnp.where(table < 0, 0, table // LANES)
    steps = jnp.arange(max(TAIL, MOVES), dtype=I32)
    tail_hit = tail_at[:, None, :] == steps[None, :TAIL, None]
    tails = jnp.max(jnp.where(tail_hit, ids[None, None, :], -1), axis=2)
    move_hit = (rank - keep[:, None])[:, None, :] == steps[None, :MOVES, None]
    moves = jnp.max(jnp.where(move_hit, ids[None, None, :], 0), axis=2)
    last_load = jnp.max(jnp.where((at == n_round - 1) & in_round, load, 0))
    return experts, sources, tails, moves, n_round, last_load


def solution(mesh):
    n_group, n_data = mesh.shape["expert"], mesh.shape["data"]
    assert n_group == 4 and n_data == 2
    tok_spec = P(("rep", "expert", "data"), None)
    wide_spec = P("expert", "data", None)
    down_spec = P("expert", None, "data")
    swap = [(0, 1), (1, 0)]

    def across(value, k):
        return lax.ppermute(value, "expert", [(p, p ^ k) for p in range(n_group)])

    def spread(groups):
        return (groups[0],) + tuple(across(groups[k], k) for k in range(1, n_group))

    def swapped(parts):
        return tuple(lax.ppermute(part, "data", swap) for part in parts)

    def device_body(x_loc, idx_loc, gate_loc, wg_loc, wu_loc, wd_loc):
        tok_rows, d_model = x_loc.shape
        top_k = idx_loc.shape[1]
        n_local = wg_loc.shape[0]
        n_exp = n_local * n_group
        capacity = capacity_rows(tok_rows, top_k, n_exp)
        me, q = lax.axis_index("expert"), lax.axis_index("data")
        weights = (wg_loc, wu_loc, wd_loc)
        slot, slot_t, gate_te, tile_starts, count = route(idx_loc.T, gate_loc.T, capacity)
        starts = jnp.concatenate([tile_starts[:, 0], count[:1]], axis=0)
        counts = lax.all_gather(count[0, :n_exp], ("expert", "data"))
        experts, sources, tails, moves, n_round, last_load = plan(counts, n_group)
        mine = me ^ jnp.arange(n_group, dtype=I32)
        table = jnp.concatenate([jnp.full((1, n_group), NO_EXPERT, I32), experts[mine].T], axis=0)
        my_sources = sources[me]
        my_hot = (experts[me][:, None] == jnp.arange(n_exp, dtype=I32)[None, :]).astype(I32)
        my_counts = counts.reshape(n_group, n_data, n_exp)[mine, q]
        used = jnp.sum(my_hot[:, None, :] * my_counts[None, :, :], axis=2)
        tail_local = jnp.maximum(tails[me], 0)
        tail_global = jnp.where(tails < 0, NO_EXPERT, tails + n_local * jnp.arange(n_group, dtype=I32)[:, None])[mine]

        def slices(e, source=None):
            return tuple(lax.dynamic_index_in_dim(w, e, axis=0, keepdims=False) for w in source or weights)

        def outgoing(r):
            s = my_sources[r]
            kind = jnp.maximum(s - n_local + 1, 0)
            return lax.switch(kind, [lambda: slices(jnp.minimum(s, n_local - 1))] + [lambda i=i: extras[i] for i in range(MOVES)])

        def one_round(r, carry, tag):
            token, peer, rows, back, send, acc = carry
            peer_next = swapped(send)
            *picked, token = pick(r + 1 + token, table, starts, slot_t, x_loc, capacity)
            rows_next = spread(picked)
            out_rows, token = expert_ffn(r + token, my_sources, used, weights, extras, peer, rows)
            back_next = spread(out_rows)
            send_next, token = lax.optimization_barrier((outgoing(r[0] + 2 + token[0]), token)) if not tag.endswith("1") else (None, token)
            acc, token = mix(r - 1 + token, table, starts, slot, gate_te, back, acc, F32)
            return token, peer_next, rows_next, back_next, send_next, acc

        half = d_model // n_data
        peer = swapped(slices(my_sources[0]))
        *picked, token = pick(jnp.zeros((1,), I32), table, starts, slot_t, x_loc, capacity)
        rows = spread(picked)
        later, token = lax.optimization_barrier((weights, token))
        extras = tuple(tuple(across(part, 1) for part in slices(moves[me, i] + token[0], later)) for i in range(MOVES))
        tail_picked, token = lax.optimization_barrier((tuple(pick_tail(tail_global + token, slot_t, x_loc)), token))
        tail_rows = spread(tail_picked)
        later, token = lax.optimization_barrier((weights, token))
        send = slices(my_sources[1] + token[0], later)
        blank = tuple(unset(*[jax.ShapeDtypeStruct((capacity, d_model), BF16)] * n_group))
        carry = (token, peer, rows, blank, send, x_loc.astype(F32))
        tail_x = jnp.stack([group.reshape(TAIL, TAIL_CAP, d_model) for group in tail_rows], axis=1).reshape(TAIL, n_group * TAIL_CAP, d_model)
        tail_mine = lax.dynamic_slice_in_dim(tail_x, q * half, half, axis=2)
        tail_peer = lax.ppermute(lax.dynamic_slice_in_dim(tail_x, (1 - q) * half, half, axis=2), "data", swap)

        odd = n_round % 2

        def two_rounds(i, c):
            r = jnp.full((1,), 2 * i, I32)
            return one_round(r + 1, one_round(r, c, "a"), "b")

        carry = lax.fori_loop(0, (n_round - 2) // 2, two_rounds, carry)
        last = jnp.full((1,), n_round - 1, I32)
        ffn = wg_loc.shape[2]

        def diagonal(value, k):
            pairs = [(s * n_group + p, (1 - s) * n_group + (p ^ k)) for p in range(n_group) for s in range(n_data)]
            return lax.ppermute(value, ("data", "expert"), pairs)

        def finish(n_peel):
            def run():
                state = carry
                for left in range(n_peel, 0, -1):
                    state = one_round(last - left, state, f"peel{n_peel}{left}")
                token, peer, rows, back, _, acc = state
                (partial, partial_peer), token = lax.optimization_barrier((tuple(tail_in(tail_local + token, tail_mine, tail_peer, wg_loc, wu_loc)), token))
                partial_peer = lax.ppermute(partial_peer, "data", swap)
                hidden, token = ffn_up(last + token, my_sources, used, weights, extras, peer, rows)
                out_first, out_others, token = ffn_down(last + token, my_sources, used, weights, extras, peer, hidden)
                back_first = spread(out_first)
                acc, token = mix(last - 1 + token, table, starts, slot, gate_te, back, acc, F32)
                (partial, partial_peer), token = lax.optimization_barrier(((partial, partial_peer), token))
                partial_sum = partial + partial_peer
                tail_h = (jax.nn.silu(partial_sum[..., :ffn]) * partial_sum[..., ffn:]).astype(BF16)
                tail_h_peer = lax.ppermute(tail_h, "data", swap)
                mine, theirs = tail_out(tail_local + token, tail_h, tail_h_peer, wd_loc)
                mine, theirs = (o.reshape(TAIL, n_group, TAIL_CAP, half) for o in (mine, theirs))
                tail_halves = []
                for k in range(n_group):
                    near, far = mine[:, k].reshape(TAIL * TAIL_CAP, half), theirs[:, k].reshape(TAIL * TAIL_CAP, half)
                    tail_halves.append((across(near, k) if k else near, diagonal(far, k)))
                near, far = (jnp.concatenate(parts, axis=0) for parts in zip(*tail_halves))
                tail_back = jnp.where(q == 0, jnp.concatenate([near, far], axis=1), jnp.concatenate([far, near], axis=1))
                away = tuple(out_others[1:])
                others = lax.cond(
                    last_load > LIGHT,
                    lambda: tuple(across(group, k) for k, group in enumerate(away, 1)),
                    lambda: tuple(jnp.zeros_like(group) for group in away),
                )
                back_last = list(back_first) + [out_others[0], *others]
                return mix(last + token, table, starts, slot, gate_te, back_last, acc, BF16, (tail_global, tail_back))[0]

            return run

        return lax.cond(odd == 1, finish(2), finish(1))

    return jax.shard_map(device_body, mesh=mesh, in_specs=(tok_spec, tok_spec, tok_spec, wide_spec, wide_spec, down_spec), out_specs=tok_spec, check_vma=False)
```
